8 devices in a mesh: data: 1 (over z), cols: 2 (over y), model: 4 (over x, core).
Axes of the slice: x: 2, y: 2, z: 1, core: 2. Of those that a mesh axis runs over, the one named last changes fastest.
Arguments:
- x_in: bfloat16 [32, 64, 128, 256], P('data', None, 'cols', 'model')
- w_conv1: bfloat16 [3, 3, 256, 512], P(None, None, 'model')
- b_conv1: float32 [512], replicated
- w_conv2: bfloat16 [3, 3, 512, 512], replicated
- b_conv2: float32 [512], replicated
Outputs:
- output: float32 [32, 64, 128, 512], P('data', 'model', 'cols')
All inputs are finite; a program needn't handle non-finite values.
Results may differ from the reference program's by a relative error of at most 0.00994635.
Values are sent between devices in bfloat16 or wider.
A program may use at most 1 GiB of HBM per device.

```python
import jax
import jax.numpy as jnp
from jax import lax

IMAGES = 32
HEIGHT = 64
WIDTH = 128
CHAN_IN = 256
CHAN_MID = 512
CHAN_OUT = 512
CONV_DIMS = ('NHWC', 'HWIO', 'NHWC')


def setup_inputs(seed: int = 0, part: int = 0) -> dict:
    root_key = jax.random.key(seed)
    key_x, key_w1, key_b1, key_w2, key_b2 = jax.random.split(root_key, 5)
    key_x = jax.random.fold_in(key_x, part)
    x_in = jax.random.normal(key_x, (IMAGES, HEIGHT, WIDTH, CHAN_IN), jnp.float32)
    w_conv1 = jax.random.normal(key_w1, (3, 3, CHAN_IN, CHAN_MID), jnp.float32) * (9.0 * CHAN_IN) ** -0.5
    b_conv1 = 0.5 * jax.random.normal(key_b1, (CHAN_MID,), jnp.float32)
    w_conv2 = jax.random.normal(key_w2, (3, 3, CHAN_MID, CHAN_OUT), jnp.float32) * (4.5 * CHAN_MID) ** -0.5
    b_conv2 = 0.5 * jax.random.normal(key_b2, (CHAN_OUT,), jnp.float32)
    return {'x_in': x_in.astype(jnp.bfloat16), 'w_conv1': w_conv1.astype(jnp.bfloat16), 'b_conv1': b_conv1, 'w_conv2': w_conv2.astype(jnp.bfloat16), 'b_conv2': b_conv2}


def reference(x_in, w_conv1, b_conv1, w_conv2, b_conv2):
    filt_one = w_conv1.astype(jnp.float32)
    filt_two = w_conv2.astype(jnp.float32)

    def one_image(single):
        pre_act = lax.conv_general_dilated(single[None].astype(jnp.float32), filt_one, (1, 1), 'SAME', dimension_numbers=CONV_DIMS)
        hidden = jnp.maximum(pre_act + b_conv1, 0.0).astype(jnp.bfloat16)
        result = lax.conv_general_dilated(hidden.astype(jnp.float32), filt_two, (1, 1), 'SAME', dimension_numbers=CONV_DIMS)
        return (result + b_conv2)[0]

    return lax.map(one_image, x_in)
```

```python
import functools

import jax
import jax.numpy as jnp
from jax import lax
from jax.experimental import pallas as pl
from jax.experimental.pallas import tpu as pltpu
from jax.sharding import PartitionSpec as P

ROWS = 16
COLS = 64
WIN = 20


def shift_down(v, edge):
    rolled = pltpu.roll(v, 1, axis=0)
    pos = lax.broadcasted_iota(jnp.int32, v.shape, 0) % COLS
    return jnp.where(pos == 0, edge, rolled)


def shift_up(v, edge):
    rolled = pltpu.roll(v, v.shape[0] - 1, axis=0)
    pos = lax.broadcasted_iota(jnp.int32, v.shape, 0) % COLS
    return jnp.where(pos == COLS - 1, edge, rolled)


def build_x3(is_left, xc, hx, x3, xh):
    for half in range(2):
        lane = half * 128
        for r in range(WIN):
            v = xc[half, r].astype(jnp.float32)
            h = hx[half, r].astype(jnp.float32)
            near = jnp.where(is_left, h[0:1], h[15:16])
            far = jnp.where(is_left, h[1:2], h[14:15])
            own = jnp.where(is_left, v[COLS - 1:COLS], v[0:1])
            zero = jnp.zeros_like(near)
            rows = pl.ds(r * COLS, COLS)
            x3[rows, lane:lane + 128] = shift_down(v, jnp.where(is_left, zero, near)).astype(jnp.bfloat16)
            x3[rows, 256 + lane:384 + lane] = xc[half, r]
            x3[rows, 512 + lane:640 + lane] = shift_up(v, jnp.where(is_left, near, zero)).astype(jnp.bfloat16)
            xh[r:r + 1, lane:lane + 128] = jnp.where(is_left, own, far)
            xh[r:r + 1, 256 + lane:384 + lane] = near
            xh[r:r + 1, 512 + lane:640 + lane] = jnp.where(is_left, far, own)


def conv1(is_left, top, bottom, x3, xh, w1, b1, y3, blocks=((0, 10), (10, 8))):
    edge_all = None
    for first, count in blocks:
        m = count * COLS
        lhs = jnp.concatenate([x3[(first + dy) * COLS:(first + dy) * COLS + m, :] for dy in range(3)], axis=1)
        if first == 0:
            edge = jnp.concatenate([xh[dy:dy + 32, :] for dy in range(3)], axis=1).astype(jnp.bfloat16)
            lhs = jnp.concatenate([edge, lhs], axis=0)
        z = jnp.dot(lhs, w1[...], preferred_element_type=jnp.float32)
        z = jnp.maximum(z + b1[...], 0.0)
        if first == 0:
            edge_all = z[:32]
            z = z[32:]
        for r in range(count):
            row = first + r
            v = z[r * COLS:(r + 1) * COLS]
            e = edge_all[row:row + 1]
            if row == 0:
                v = jnp.where(top, 0.0, v)
                e = jnp.where(top, 0.0, e)
            if row == ROWS + 1:
                v = jnp.where(bottom, 0.0, v)
                e = jnp.where(bottom, 0.0, e)
            zero = jnp.zeros_like(e)
            dst = pl.ds(row * COLS, COLS)
            y3[dst, 0:512] = shift_down(v, jnp.where(is_left, zero, e)).astype(jnp.bfloat16)
            y3[dst, 512:1024] = v.astype(jnp.bfloat16)
            y3[dst, 1024:1536] = shift_up(v, jnp.where(is_left, e, zero)).astype(jnp.bfloat16)


def conv2(y3, w2, b2, out, blk=8):
    for first in range(0, ROWS, blk):
        m = blk * COLS
        lhs = jnp.concatenate([y3[(first + dy) * COLS:(first + dy) * COLS + m, :] for dy in range(3)], axis=1)
        out[first * COLS:first * COLS + m, :] = jnp.dot(lhs, w2[...], preferred_element_type=jnp.float32) + b2[...]


def compute_kernel(xg, hx, w1, b1, w2, b2, out, x3, xh, y3):
    model = lax.axis_index('model')
    is_left = lax.axis_index('cols') == 0

    @pl.when(pl.program_id(0) == 0)
    def _():
        xh[...] = jnp.zeros_like(xh)

    build_x3(is_left, xg.at[0], hx.at[0], x3, xh)
    conv1(is_left, model == 0, model == 3, x3, xh, w1, b1, y3)
    conv2(y3, w2, b2, out.at[0])


def compute(xg, hx, w1, b1, w2, b2):
    images = xg.shape[0]
    full = lambda shape: pl.BlockSpec(shape, lambda n: (0,) * len(shape))
    return pl.pallas_call(
        compute_kernel,
        grid=(images,),
        out_shape=jax.ShapeDtypeStruct((images, ROWS * COLS, 512), jnp.float32),
        in_specs=[
            pl.BlockSpec((1, 2, WIN, COLS, 128), lambda n: (n, 0, 0, 0, 0)),
            pl.BlockSpec((1, 2, WIN, 16, 128), lambda n: (n, 0, 0, 0, 0)),
            full((2304, 512)), full((1, 512)), full((4608, 512)), full((1, 512)),
        ],
        out_specs=pl.BlockSpec((1, ROWS * COLS, 512), lambda n: (n, 0, 0)),
        scratch_shapes=[
            pltpu.VMEM((WIN * COLS, 768), jnp.bfloat16),
            pltpu.VMEM((40, 768), jnp.float32),
            pltpu.VMEM(((ROWS + 2) * COLS, 1536), jnp.bfloat16),
        ],
        compiler_params=pltpu.CompilerParams(vmem_limit_bytes=60 * 1024 * 1024),
    )(xg, hx, w1, b1, w2, b2)


def solution(mesh):
    def local_step(x, w1, b1, w2, b2):
        images = x.shape[0]
        wide = jnp.pad(x, ((0, 0), (2, 2), (0, 0), (0, 0)))
        tiles = jnp.stack([wide[:, ROWS * k:ROWS * k + WIN] for k in range(4)])
        got = lax.all_to_all(tiles, 'model', 0, 0)
        got = got.reshape(2, 2, images, WIN, COLS, 64)
        xg = got.transpose(2, 0, 3, 4, 1, 5).reshape(images, 2, WIN, COLS, 128)
        is_left = lax.axis_index('cols') == 0
        edge = jnp.where(is_left, xg[:, :, :, 48:64], xg[:, :, :, 0:16])
        hx = lax.ppermute(edge, 'cols', [(0, 1), (1, 0)])
        w1g = lax.all_gather(w1, 'model', axis=2, tiled=True).reshape(2304, 512)
        y = compute(xg, hx, w1g, b1.reshape(1, 512), w2.reshape(4608, 512), b2.reshape(1, 512))
        return y.reshape(images, ROWS, COLS, 512)

    return jax.shard_map(local_step, mesh=mesh, in_specs=(P('data', None, 'cols', 'model'), P(None, None, 'model', None), P(), P(), P()), out_specs=P('data', 'model', 'cols', None), check_vma=False)
```

```python
import functools

import jax
import jax.numpy as jnp
from jax import lax
from jax.experimental import pallas as pl
from jax.experimental.pallas import tpu as pltpu
from jax.sharding import PartitionSpec as P

ROWS = 16
COLS = 64
WIN = 20
MESH = pl.DeviceIdType.MESH
SLOT_A = 2
SLOT_S = 4
SLOT_X = 8
SLOT_H = 4


def shift_down(v, edge):
    rolled = pltpu.roll(v, 1, axis=0)
    pos = lax.broadcasted_iota(jnp.int32, v.shape, 0) % COLS
    return jnp.where(pos == 0, edge, rolled)


def shift_up(v, edge):
    rolled = pltpu.roll(v, v.shape[0] - 1, axis=0)
    pos = lax.broadcasted_iota(jnp.int32, v.shape, 0) % COLS
    return jnp.where(pos == COLS - 1, edge, rolled)


def build_x3(is_left, xc, hx, x3, xh):
    for half in range(2):
        lane = half * 128
        for r in range(WIN):
            mid = xc[half, 2 + r]
            v = mid.astype(jnp.float32)
            h = hx[half, r].astype(jnp.float32)
            near = jnp.where(is_left, h[0:1], h[15:16])
            far = jnp.where(is_left, h[1:2], h[14:15])
            own = jnp.where(is_left, v[COLS - 1:COLS], v[0:1])
            zero = jnp.zeros_like(near)
            rows = pl.ds(r * COLS, COLS)
            x3[rows, lane:lane + 128] = shift_down(v, jnp.where(is_left, zero, near)).astype(jnp.bfloat16)
            x3[rows, 256 + lane:384 + lane] = mid
            x3[rows, 512 + lane:640 + lane] = shift_up(v, jnp.where(is_left, near, zero)).astype(jnp.bfloat16)
            xh[r:r + 1, lane:lane + 128] = jnp.where(is_left, own, far)
            xh[r:r + 1, 256 + lane:384 + lane] = near
            xh[r:r + 1, 512 + lane:640 + lane] = jnp.where(is_left, far, own)


def conv1(is_left, top, bottom, x3, xh, w1, b1, y3, blocks=((0, 10), (10, 8))):
    edge_all = None
    for first, count in blocks:
        m = count * COLS
        lhs = jnp.concatenate([x3[(first + dy) * COLS:(first + dy) * COLS + m, :] for dy in range(3)], axis=1)
        if first == 0:
            edge = jnp.concatenate([xh[dy:dy + 32, :] for dy in range(3)], axis=1).astype(jnp.bfloat16)
            lhs = jnp.concatenate([edge, lhs], axis=0)
        z = jnp.dot(lhs, w1[...].reshape(2304, 512), preferred_element_type=jnp.float32)
        z = jnp.maximum(z + b1[...], 0.0)
        if first == 0:
            edge_all = z[:32]
            z = z[32:]
        for r in range(count):
            row = first + r
            v = z[r * COLS:(r + 1) * COLS]
            e = edge_all[row:row + 1]
            if row == 0:
                v = jnp.where(top, 0.0, v)
                e = jnp.where(top, 0.0, e)
            if row == ROWS + 1:
                v = jnp.where(bottom, 0.0, v)
                e = jnp.where(bottom, 0.0, e)
            zero = jnp.zeros_like(e)
            dst = pl.ds(row * COLS, COLS)
            y3[dst, 0:512] = shift_down(v, jnp.where(is_left, zero, e)).astype(jnp.bfloat16)
            y3[dst, 512:1024] = v.astype(jnp.bfloat16)
            y3[dst, 1024:1536] = shift_up(v, jnp.where(is_left, e, zero)).astype(jnp.bfloat16)


def conv2(y3, w2, b2, out, blk=8):
    for first in range(0, ROWS, blk):
        m = blk * COLS
        lhs = jnp.concatenate([y3[(first + dy) * COLS:(first + dy) * COLS + m, :] for dy in range(3)], axis=1)
        out[first * COLS:first * COLS + m, :] = jnp.dot(lhs, w2[...], preferred_element_type=jnp.float32) + b2[...]


def merge(slot, chip, off, ab, xc_slot, sb_slot):
    for r in range(WIN):
        xc_slot[chip, off + r] = jnp.concatenate([ab[slot, 0, 0, r], ab[slot, 0, 1, r]], axis=-1)
        sb_slot[r] = jnp.concatenate([ab[slot, 1, 0, r], ab[slot, 1, 1, r]], axis=-1)


def fused_kernel(images, x, w1, b1, w2, b2, y, ab, sb, xc, hx, x3, xh, y3, ob, w1v, w2v,
                 loc_sem, a_send, a_recv, x_send, x_recv, h_send, h_recv, o_sem, w_loc, w_send, w_recv,
                 credit_a, credit_x, credit_h):
    data = lax.axis_index('data')
    side = lax.axis_index('cols')
    model = lax.axis_index('model')
    is_left = side == 0
    chip = model // 2
    core = model % 2
    mate = chip * 2 + 1 - core
    far = (1 - chip) * 2 + core
    far_mate = (1 - chip) * 2 + 1 - core
    to_mate = (data, side, mate)
    to_far = (data, side, far)
    to_side = (data, 1 - side, model)

    def source(m):
        return jnp.where(m == 0, 0, jnp.where(m == 3, 44, ROWS * m - 2))

    def place(m):
        return jnp.where(m == 0, 4, jnp.where(m == 3, 0, 2))

    edge = pl.multiple_of(jnp.where(is_left, COLS - 16, 0), 16)

    for slot in range(SLOT_X):
        for half in range(2):
            for row in (2, 3, 20, 21):
                xc[slot, half, row] = jnp.zeros((COLS, 128), jnp.bfloat16)
    xh[...] = jnp.zeros_like(xh)

    barrier = pltpu.get_barrier_semaphore()
    for peer in (to_mate, to_far, to_side):
        pl.semaphore_signal(barrier, inc=1, device_id=peer, device_id_type=MESH)
    pl.semaphore_wait(barrier, 3)

    def remote(src, dst, send, recv, peer):
        return pltpu.make_async_remote_copy(src_ref=src, dst_ref=dst, send_sem=send, recv_sem=recv, device_id=peer, device_id_type=MESH)

    def w1_part(m):
        return w1v.at[:, pl.ds(pl.multiple_of(m * 64, 64), 64), :]

    w_far = remote(w1, w1_part(model), w_send.at[0], w_recv.at[0], to_far)
    w_mate = remote(w1, w1_part(model), w_send.at[1], w_recv.at[1], to_mate)
    w_pass = remote(w1_part(far), w1_part(far), w_send.at[2], w_recv.at[2], to_mate)
    w_own = pltpu.make_async_copy(w1, w1_part(model), w_loc.at[0])
    w2_own = pltpu.make_async_copy(w2, w2v, w_loc.at[1])

    def own_copy(n, win):
        slot = n % SLOT_A
        rows = pl.ds(source(model if win == 0 else far), WIN)
        return pltpu.make_async_copy(x.at[n, rows], ab.at[slot, win, core], loc_sem.at[slot, win])

    def mate_copy(n, win):
        slot = n % SLOT_A
        rows = pl.ds(source(mate if win == 0 else far_mate), WIN)
        return remote(x.at[n, rows], ab.at[slot, win, core], a_send.at[slot, win], a_recv.at[slot, win], to_mate)

    def far_copy(n):
        slot = n % SLOT_X
        return remote(sb.at[n % SLOT_S], xc.at[slot, chip, pl.ds(place(far), WIN)], x_send.at[slot], x_recv.at[slot], to_far)

    def far_land(n):
        slot = n % SLOT_X
        return remote(sb.at[n % SLOT_S], xc.at[slot, 1 - chip, pl.ds(place(model), WIN)], x_send.at[slot], x_recv.at[slot], to_far)

    def side_copy(n):
        slot = n % SLOT_H
        return remote(xc.at[n % SLOT_X, :, pl.ds(2, WIN), pl.ds(edge, 16), :], hx.at[slot], h_send.at[slot], h_recv.at[slot], to_side)

    def out_copy(n):
        return pltpu.make_async_copy(ob.at[n % 2], y.at[n], o_sem.at[n % 2])

    def within(n):
        return jnp.logical_and(n >= 0, n < images)

    def control(i):
        na, nm, nx, nh, nb = i + 6, i + 5, i + 4, i + 2, i + 1

        @pl.when(within(na))
        def _():
            @pl.when(na >= SLOT_A)
            def _():
                pl.semaphore_wait(credit_a, 1)
            for win in range(2):
                own_copy(na, win).start()
                mate_copy(na, win).start()

        @pl.when(within(nx))
        def _():
            @pl.when(nx >= SLOT_X)
            def _():
                pl.semaphore_wait(credit_x, 1)
            far_copy(nx).start()

        @pl.when(within(nm))
        def _():
            for win in range(2):
                own_copy(nm, win).wait()
                mate_copy(nm, win).wait()

        @pl.when(within(nh))
        def _():
            far_copy(nh).wait_send()
            far_land(nh).wait_recv()

            @pl.when(nh >= SLOT_H)
            def _():
                pl.semaphore_wait(credit_h, 1)
            side_copy(nh).start()

        @pl.when(within(nb))
        def _():
            side_copy(nb).wait()

    def release(i):
        nm, nb = i + 5, i + 1

        @pl.when(jnp.logical_and(nm >= 0, nm < images - SLOT_A))
        def _():
            pl.semaphore_signal(credit_a, inc=1, device_id=to_mate, device_id_type=MESH)

        @pl.when(jnp.logical_and(nb >= 0, nb < images - SLOT_X))
        def _():
            pl.semaphore_signal(credit_x, inc=1, device_id=to_far, device_id_type=MESH)

        @pl.when(jnp.logical_and(nb >= 0, nb < images - SLOT_H))
        def _():
            pl.semaphore_signal(credit_h, inc=1, device_id=to_side, device_id_type=MESH)

    def do_merge(n):
        merge(n % SLOT_A, chip, place(model), ab, xc.at[n % SLOT_X], sb.at[n % SLOT_S])

    def do_build(n):
        build_x3(is_left, xc.at[n % SLOT_X], hx.at[n % SLOT_H], x3, xh)

    w_far.start()
    w_mate.start()
    w_own.start()
    w2_own.start()

    def fill(t, _):
        i = t - 6
        control(i)

        @pl.when(within(i + 5))
        def _():
            do_merge(i + 5)

        @pl.when(within(i + 1))
        def _():
            do_build(i + 1)
        release(i)
        return 0

    lax.fori_loop(0, 6, fill, 0)
    w_far.wait()
    w_pass.start()
    w_mate.wait()
    w_own.wait()
    w2_own.wait()
    w_pass.wait()

    def step(i, _):
        control(i)

        @pl.when(i >= 2)
        def _():
            out_copy(i - 2).wait()
        conv1(is_left, model == 0, model == 3, x3, xh, w1v, b1, y3)
        do_build(jnp.minimum(i + 1, images - 1))
        do_merge(i + 5)
        conv2(y3, w2v, b2, ob.at[i % 2])
        out_copy(i).start()
        release(i)
        return 0

    lax.fori_loop(0, images, step, 0)
    out_copy(images - 2).wait()
    out_copy(images - 1).wait()


def fused(x, w1, b1, w2, b2):
    images = x.shape[0]
    hbm = pl.BlockSpec(memory_space=pl.ANY)
    vmem = pl.BlockSpec(memory_space=pltpu.VMEM)
    dma = pltpu.SemaphoreType.DMA
    bf16 = jnp.bfloat16
    return pl.pallas_call(
        functools.partial(fused_kernel, images),
        out_shape=jax.ShapeDtypeStruct((images, ROWS * COLS, 512), jnp.float32),
        in_specs=[hbm, hbm, vmem, hbm, vmem],
        out_specs=hbm,
        scratch_shapes=[
            pltpu.VMEM((SLOT_A, 2, 2, WIN, COLS, 64), bf16),
            pltpu.VMEM((SLOT_S, WIN, COLS, 128), bf16),
            pltpu.VMEM((SLOT_X, 2, WIN + 4, COLS, 128), bf16),
            pltpu.VMEM((SLOT_H, 2, WIN, 16, 128), bf16),
            pltpu.VMEM((WIN * COLS, 768), bf16),
            pltpu.VMEM((40, 768), jnp.float32),
            pltpu.VMEM(((ROWS + 2) * COLS, 1536), bf16),
            pltpu.VMEM((2, ROWS * COLS, 512), jnp.float32),
            pltpu.VMEM((9, 256, 512), bf16),
            pltpu.VMEM((4608, 512), bf16),
            dma((SLOT_A, 2)), dma((SLOT_A, 2)), dma((SLOT_A, 2)),
            dma((SLOT_X,)), dma((SLOT_X,)), dma((SLOT_H,)), dma((SLOT_H,)), dma((2,)),
            dma((2,)), dma((3,)), dma((3,)),
            pltpu.SemaphoreType.REGULAR, pltpu.SemaphoreType.REGULAR, pltpu.SemaphoreType.REGULAR,
        ],
        compiler_params=pltpu.CompilerParams(vmem_limit_bytes=60 * 1024 * 1024, collective_id=0, has_side_effects=True),
    )(x, w1, b1, w2, b2)


def solution(mesh):
    def local_step(x, w1, b1, w2, b2):
        images = x.shape[0]
        y = fused(x, w1.reshape(9, 64, 512), b1.reshape(1, 512), w2.reshape(4608, 512), b2.reshape(1, 512))
        return y.reshape(images, ROWS, COLS, 512)

    return jax.shard_map(local_step, mesh=mesh, in_specs=(P('data', None, 'cols', 'model'), P(None, None, 'model', None), P(), P(), P()), out_specs=P('data', 'model', 'cols', None), check_vma=False)
```

```python
import functools

import jax
import jax.numpy as jnp
from jax import lax
from jax.experimental import pallas as pl
from jax.experimental.pallas import tpu as pltpu
from jax.sharding import PartitionSpec as P

ROWS = 16
COLS = 64
WIN = 20
MESH = pl.DeviceIdType.MESH
SLOT_A = 4
SLOT_S = 8
SLOT_X = 16
SLOT_H = 8
LATER = 6


def shift_down(v, edge):
    rolled = pltpu.roll(v, 1, axis=0)
    pos = lax.broadcasted_iota(jnp.int32, v.shape, 0) % COLS
    return jnp.where(pos == 0, edge, rolled)


def shift_up(v, edge):
    rolled = pltpu.roll(v, v.shape[0] - 1, axis=0)
    pos = lax.broadcasted_iota(jnp.int32, v.shape, 0) % COLS
    return jnp.where(pos == COLS - 1, edge, rolled)


def build_x3(is_left, xc, hx, x3, xh):
    for half in range(2):
        lane = half * 128
        for r in range(WIN):
            mid = xc[half, 2 + r]
            v = mid.astype(jnp.float32)
            h = hx[half, r].astype(jnp.float32)
            near = jnp.where(is_left, h[0:1], h[15:16])
            far = jnp.where(is_left, h[1:2], h[14:15])
            own = jnp.where(is_left, v[COLS - 1:COLS], v[0:1])
            zero = jnp.zeros_like(near)
            rows = pl.ds(r * COLS, COLS)
            x3[rows, lane:lane + 128] = shift_down(v, jnp.where(is_left, zero, near)).astype(jnp.bfloat16)
            x3[rows, 256 + lane:384 + lane] = mid
            x3[rows, 512 + lane:640 + lane] = shift_up(v, jnp.where(is_left, near, zero)).astype(jnp.bfloat16)
            xh[r:r + 1, lane:lane + 128] = jnp.where(is_left, own, far)
            xh[r:r + 1, 256 + lane:384 + lane] = near
            xh[r:r + 1, 512 + lane:640 + lane] = jnp.where(is_left, far, own)


def conv1(is_left, top, bottom, x3, xh, w1, b1, y3, blocks=((0, 10), (10, 8))):
    edge_all = None
    for first, count in blocks:
        m = count * COLS
        lhs = jnp.concatenate([x3[(first + dy) * COLS:(first + dy) * COLS + m, :] for dy in range(3)], axis=1)
        if first == 0:
            edge = jnp.concatenate([xh[dy:dy + 32, :] for dy in range(3)], axis=1).astype(jnp.bfloat16)
            lhs = jnp.concatenate([edge, lhs], axis=0)
        z = jnp.dot(lhs, w1[...].reshape(2304, 512), preferred_element_type=jnp.float32)
        z = jnp.maximum(z + b1[...], 0.0)
        if first == 0:
            edge_all = z[:32]
            z = z[32:]
        for r in range(count):
            row = first + r
            v = z[r * COLS:(r + 1) * COLS]
            e = edge_all[row:row + 1]
            if row == 0:
                v = jnp.where(top, 0.0, v)
                e = jnp.where(top, 0.0, e)
            if row == ROWS + 1:
                v = jnp.where(bottom, 0.0, v)
                e = jnp.where(bottom, 0.0, e)
            zero = jnp.zeros_like(e)
            dst = pl.ds(row * COLS, COLS)
            y3[dst, 0:512] = shift_down(v, jnp.where(is_left, zero, e)).astype(jnp.bfloat16)
            y3[dst, 512:1024] = v.astype(jnp.bfloat16)
            y3[dst, 1024:1536] = shift_up(v, jnp.where(is_left, e, zero)).astype(jnp.bfloat16)


def conv2(y3, w2, b2, out, blk=8):
    for first in range(0, ROWS, blk):
        m = blk * COLS
        lhs = jnp.concatenate([y3[(first + dy) * COLS:(first + dy) * COLS + m, :] for dy in range(3)], axis=1)
        out[first * COLS:first * COLS + m, :] = jnp.dot(lhs, w2[...], preferred_element_type=jnp.float32) + b2[...]


def merge(slot, chip, off, ab, xc_slot, sb_slot):
    for r in range(WIN):
        xc_slot[chip, off + r] = jnp.concatenate([ab[slot, 0, 0, r], ab[slot, 0, 1, r]], axis=-1)
        sb_slot[r] = jnp.concatenate([ab[slot, 1, 0, r], ab[slot, 1, 1, r]], axis=-1)


def fused_kernel(images, x, w1, b1, w2, b2, y, x_rest, h_rest, w1_all, ab, sb, xc, hx, x3, xh, y3, ob, w1v, w2v,
                 loc_sem, a_send, a_recv, x_send, x_recv, h_send, h_recv, o_sem, w_loc, w_send, w_recv, rest_sem,
                 credit_a, credit_x, credit_h):
    now = images - LATER
    data = lax.axis_index('data')
    side = lax.axis_index('cols')
    model = lax.axis_index('model')
    is_left = side == 0
    chip = model // 2
    core = model % 2
    mate = chip * 2 + 1 - core
    far = (1 - chip) * 2 + core
    far_mate = (1 - chip) * 2 + 1 - core
    to_mate = (data, side, mate)
    to_far = (data, side, far)
    to_side = (data, 1 - side, model)

    def source(m):
        return jnp.where(m == 0, 0, jnp.where(m == 3, 44, ROWS * m - 2))

    def place(m):
        return jnp.where(m == 0, 4, jnp.where(m == 3, 0, 2))

    edge = pl.multiple_of(jnp.where(is_left, COLS - 16, 0), 16)

    for slot in range(SLOT_X):
        for half in range(2):
            for row in (2, 3, 20, 21):
                xc[slot, half, row] = jnp.zeros((COLS, 128), jnp.bfloat16)
    xh[...] = jnp.zeros_like(xh)

    barrier = pltpu.get_barrier_semaphore()
    for peer in (to_mate, to_far, to_side):
        pl.semaphore_signal(barrier, inc=1, device_id=peer, device_id_type=MESH)
    pl.semaphore_wait(barrier, 3)

    def remote(src, dst, send, recv, peer):
        return pltpu.make_async_remote_copy(src_ref=src, dst_ref=dst, send_sem=send, recv_sem=recv, device_id=peer, device_id_type=MESH)

    def w1_part(m):
        return w1v.at[:, pl.ds(pl.multiple_of(m * 64, 64), 64), :]

    w_far = remote(w1, w1_part(model), w_send.at[0], w_recv.at[0], to_far)
    w_mate = remote(w1, w1_part(model), w_send.at[1], w_recv.at[1], to_mate)
    w_pass = remote(w1_part(far), w1_part(far), w_send.at[2], w_recv.at[2], to_mate)
    w_own = pltpu.make_async_copy(w1, w1_part(model), w_loc.at[0])
    w2_own = pltpu.make_async_copy(w2, w2v, w_loc.at[1])

    def own_copy(n, win):
        slot = n % SLOT_A
        rows = pl.ds(source(model if win == 0 else far), WIN)
        return pltpu.make_async_copy(x.at[n, rows], ab.at[slot, win, core], loc_sem.at[slot, win])

    def mate_copy(n, win):
        slot = n % SLOT_A
        rows = pl.ds(source(mate if win == 0 else far_mate), WIN)
        return remote(x.at[n, rows], ab.at[slot, win, core], a_send.at[slot, win], a_recv.at[slot, win], to_mate)

    def is_edge(m):
        return jnp.logical_or(m == 0, m == 3)

    def by_size(m, run):
        @pl.when(is_edge(m))
        def _():
            run(WIN - 2, jnp.where(m == 3, 2, 0))

        @pl.when(jnp.logical_not(is_edge(m)))
        def _():
            run(WIN, 0)

    def far_copy(n, m, half, count, first):
        slot = n % SLOT_X
        return remote(sb.at[n % SLOT_S, pl.ds(first, count)], xc.at[slot, half, pl.ds(place(m) + first, count)],
                      x_send.at[slot], x_recv.at[slot], to_far)

    def side_copy(n):
        slot = n % SLOT_H
        return remote(xc.at[n % SLOT_X, :, pl.ds(2, WIN), pl.ds(edge, 16), :], hx.at[slot], h_send.at[slot], h_recv.at[slot], to_side)

    def out_copy(n):
        return pltpu.make_async_copy(ob.at[n % 2], y.at[n], o_sem.at[n % 2])

    def rest_copy(n, part):
        if part == 0:
            return pltpu.make_async_copy(xc.at[n % SLOT_X, :, pl.ds(2, WIN)], x_rest.at[n - now], rest_sem.at[n - now, 0])
        return pltpu.make_async_copy(hx.at[n % SLOT_H], h_rest.at[n - now], rest_sem.at[n - now, 1])

    def last(i):
        return jnp.clip(i + 6 + jnp.maximum(i, 0) // 4, -1, images - 1)

    def each(i, run):
        lo, hi = last(i - 1), last(i)

        @pl.when(hi > lo)
        def _():
            run(lo + 1)

        @pl.when(hi > lo + 1)
        def _():
            run(lo + 2)

    def start_a(n):
        @pl.when(n >= SLOT_A)
        def _():
            pl.semaphore_wait(credit_a, 1)
        for win in range(2):
            own_copy(n, win).start()
            mate_copy(n, win).start()

    def start_x(n):
        @pl.when(n >= SLOT_X)
        def _():
            pl.semaphore_wait(credit_x, 1)
        by_size(far, lambda count, first: far_copy(n, far, chip, count, first).start())

    def wait_a(n):
        for win in range(2):
            own_copy(n, win).wait()
            mate_copy(n, win).wait()

    def start_h(n):
        by_size(far, lambda count, first: far_copy(n, far, chip, count, first).wait_send())
        by_size(model, lambda count, first: far_copy(n, model, 1 - chip, count, first).wait_recv())

        @pl.when(n >= SLOT_H)
        def _():
            pl.semaphore_wait(credit_h, 1)
        side_copy(n).start()

    def wait_h(n):
        side_copy(n).wait()

        @pl.when(n >= now)
        def _():
            rest_copy(n, 0).start()
            rest_copy(n, 1).start()

    def control(i):
        each(i, start_a)
        each(i - 2, start_x)
        each(i - 1, wait_a)

        @pl.when(last(i - 1) > last(i - 2) + 1)
        def _():
            do_merge(last(i - 1) - 1, True)
        each(i - 4, start_h)
        each(i - 5, wait_h)

    def release(i):
        def free_a(n):
            @pl.when(n < images - SLOT_A)
            def _():
                pl.semaphore_signal(credit_a, inc=1, device_id=to_mate, device_id_type=MESH)
        each(i - 1, free_a)
        built = i + 1

        @pl.when(jnp.logical_and(built >= 0, built < images - SLOT_X))
        def _():
            pl.semaphore_signal(credit_x, inc=1, device_id=to_far, device_id_type=MESH)

        @pl.when(jnp.logical_and(built >= 0, built < images - SLOT_H))
        def _():
            pl.semaphore_signal(credit_h, inc=1, device_id=to_side, device_id_type=MESH)

    def do_merge(n, live):
        merge(n % SLOT_A, chip, place(model), ab, xc.at[jnp.where(live, n % SLOT_X, SLOT_X)], sb.at[jnp.where(live, n % SLOT_S, SLOT_S)])

    def do_build(n):
        build_x3(is_left, xc.at[n % SLOT_X], hx.at[n % SLOT_H], x3, xh)

    w_far.start()
    w_mate.start()
    w_own.start()
    w2_own.start()

    def fill(t, _):
        i = t - 6
        control(i)

        @pl.when(last(i - 1) > last(i - 2))
        def _():
            do_merge(last(i - 1), True)

        @pl.when(i + 1 >= 0)
        def _():
            do_build(i + 1)
        release(i)
        return 0

    lax.fori_loop(0, 6, fill, 0)
    w_far.wait()
    w_pass.start()
    w_mate.wait()
    w_own.wait()
    w2_own.wait()
    w_pass.wait()
    w_out = pltpu.make_async_copy(w1v, w1_all, w_loc.at[2])
    w_out.start()

    def step(i, _):
        control(i)

        @pl.when(i >= 2)
        def _():
            out_copy(i - 2).wait()
        conv1(is_left, model == 0, model == 3, x3, xh, w1v, b1, y3)
        do_build(i + 1)
        do_merge(last(i - 1), last(i - 1) > last(i - 2))
        conv2(y3, w2v, b2, ob.at[i % 2])
        out_copy(i).start()
        release(i)
        return 0

    lax.fori_loop(0, now, step, 0)
    out_copy(now - 2).wait()
    out_copy(now - 1).wait()
    w_out.wait()
    for n in range(now, images):
        rest_copy(n, 0).wait()
        rest_copy(n, 1).wait()


def rest_kernel(images, y_done, x_rest, h_rest, w1, b1, w2, b2, y, xc, hx, x3, xh, y3, ob, w1v, w2v, cb,
                l_sem, w_sem, o_sem, in_sem, out_sem):
    done = images - LATER
    sets = LATER - 1
    size = -(-done // sets)
    model = lax.axis_index('model')
    is_left = lax.axis_index('cols') == 0
    weights = [pltpu.make_async_copy(w1, w1v, w_sem.at[0]), pltpu.make_async_copy(w2, w2v, w_sem.at[1])]
    xh[...] = jnp.zeros_like(xh)

    def load(n):
        return [pltpu.make_async_copy(x_rest.at[n], xc.at[n, :, pl.ds(2, WIN)], l_sem.at[n, 0]),
                pltpu.make_async_copy(h_rest.at[n], hx.at[n], l_sem.at[n, 1])]

    def bring(s, q):
        return pltpu.make_async_copy(y_done.at[s + sets * q], cb.at[s % 2, q], in_sem.at[s % 2, q])

    def put(s, q):
        return pltpu.make_async_copy(cb.at[s % 2, q], y.at[s + sets * q], out_sem.at[s % 2, q])

    def each(s, run):
        for q in range(size):
            @pl.when(jnp.logical_and(jnp.logical_and(s >= 0, s < sets), s + sets * q < done))
            def _():
                run(s, q)

    def out_copy(n):
        return pltpu.make_async_copy(ob.at[n % 2], y.at[done + n], o_sem.at[n % 2])

    for copy in load(0) + weights[:1] + load(1) + weights[1:] + [c for n in range(2, LATER) for c in load(n)]:
        copy.start()
    for copy in load(0):
        copy.wait()
    build_x3(is_left, xc.at[0], hx.at[0], x3, xh)
    for copy in weights + [c for n in range(1, LATER) for c in load(n)]:
        copy.wait()

    def step(i, _):
        each(i - 1, lambda s, q: bring(s, q).wait())
        each(i - 1, lambda s, q: put(s, q).start())
        each(i - 2, lambda s, q: put(s, q).wait())
        each(i, lambda s, q: bring(s, q).start())

        @pl.when(i >= 2)
        def _():
            out_copy(i - 2).wait()
        conv1(is_left, model == 0, model == 3, x3, xh, w1v, b1, y3)
        n = jnp.minimum(i + 1, LATER - 1)
        build_x3(is_left, xc.at[n], hx.at[n], x3, xh)
        conv2(y3, w2v, b2, ob.at[i % 2])
        out_copy(i).start()
        return 0

    lax.fori_loop(0, LATER, step, 0)
    each(jnp.int32(sets - 1), lambda s, q: put(s, q).wait())
    out_copy(LATER - 2).wait()
    out_copy(LATER - 1).wait()


def rest(images, y_done, x_rest, h_rest, w1, b1, w2, b2):
    hbm = pl.BlockSpec(memory_space=pl.ANY)
    vmem = pl.BlockSpec(memory_space=pltpu.VMEM)
    dma = pltpu.SemaphoreType.DMA
    bf16 = jnp.bfloat16
    size = -(-(images - LATER) // (LATER - 1))
    return pl.pallas_call(
        functools.partial(rest_kernel, images),
        out_shape=jax.ShapeDtypeStruct((images, ROWS * COLS, 512), jnp.float32),
        in_specs=[hbm, hbm, hbm, hbm, vmem, hbm, vmem],
        out_specs=hbm,
        scratch_shapes=[
            pltpu.VMEM((LATER, 2, WIN + 4, COLS, 128), bf16),
            pltpu.VMEM((LATER, 2, WIN, 16, 128), bf16),
            pltpu.VMEM((WIN * COLS, 768), bf16),
            pltpu.VMEM((40, 768), jnp.float32),
            pltpu.VMEM(((ROWS + 2) * COLS, 1536), bf16),
            pltpu.VMEM((2, ROWS * COLS, 512), jnp.float32),
            pltpu.VMEM((9, 256, 512), bf16),
            pltpu.VMEM((4608, 512), bf16),
            pltpu.VMEM((2, size, ROWS * COLS, 512), jnp.float32),
            dma((LATER, 2)), dma((2,)), dma((2,)), dma((2, size)), dma((2, size)),
        ],
        compiler_params=pltpu.CompilerParams(vmem_limit_bytes=62 * 1024 * 1024),
    )(y_done, x_rest, h_rest, w1, b1, w2, b2)


def fused(x, w1, b1, w2, b2):
    images = x.shape[0]
    hbm = pl.BlockSpec(memory_space=pl.ANY)
    vmem = pl.BlockSpec(memory_space=pltpu.VMEM)
    dma = pltpu.SemaphoreType.DMA
    bf16 = jnp.bfloat16
    return pl.pallas_call(
        functools.partial(fused_kernel, images),
        out_shape=[
            jax.ShapeDtypeStruct((images - LATER, ROWS * COLS, 512), jnp.float32),
            jax.ShapeDtypeStruct((LATER, 2, WIN, COLS, 128), bf16),
            jax.ShapeDtypeStruct((LATER, 2, WIN, 16, 128), bf16),
            jax.ShapeDtypeStruct((9, 256, 512), bf16),
        ],
        in_specs=[hbm, hbm, vmem, hbm, vmem],
        out_specs=[hbm] * 4,
        scratch_shapes=[
            pltpu.VMEM((SLOT_A, 2, 2, WIN, COLS, 64), bf16),
            pltpu.VMEM((SLOT_S + 1, WIN, COLS, 128), bf16),
            pltpu.VMEM((SLOT_X + 1, 2, WIN + 4, COLS, 128), bf16),
            pltpu.VMEM((SLOT_H, 2, WIN, 16, 128), bf16),
            pltpu.VMEM((WIN * COLS, 768), bf16),
            pltpu.VMEM((40, 768), jnp.float32),
            pltpu.VMEM(((ROWS + 2) * COLS, 1536), bf16),
            pltpu.VMEM((2, ROWS * COLS, 512), jnp.float32),
            pltpu.VMEM((9, 256, 512), bf16),
            pltpu.VMEM((4608, 512), bf16),
            dma((SLOT_A, 2)), dma((SLOT_A, 2)), dma((SLOT_A, 2)),
            dma((SLOT_X,)), dma((SLOT_X,)), dma((SLOT_H,)), dma((SLOT_H,)), dma((2,)),
            dma((3,)), dma((3,)), dma((3,)), dma((LATER, 2)),
            pltpu.SemaphoreType.REGULAR, pltpu.SemaphoreType.REGULAR, pltpu.SemaphoreType.REGULAR,
        ],
        compiler_params=pltpu.CompilerParams(vmem_limit_bytes=60 * 1024 * 1024, collective_id=0, has_side_effects=True),
    )(x, w1, b1, w2, b2)


def solution(mesh):
    def local_step(x, w1, b1, w2, b2):
        images = x.shape[0]
        b1, w2, b2 = b1.reshape(1, 512), w2.reshape(4608, 512), b2.reshape(1, 512)
        done, x_rest, h_rest, w1_all = fused(x, w1.reshape(9, 64, 512), b1, w2, b2)
        y = rest(images, done, x_rest, h_rest, w1_all, b1, w2, b2)
        return y.reshape(images, ROWS, COLS, 512)

    return jax.shard_map(local_step, mesh=mesh, in_specs=(P('data', None, 'cols', 'model'), P(None, None, 'model', None), P(), P(), P()), out_specs=P('data', 'model', 'cols', None), check_vma=False)
```

```python
import functools

import jax
import jax.numpy as jnp
from jax import lax
from jax.experimental import pallas as pl
from jax.experimental.pallas import tpu as pltpu
from jax.sharding import PartitionSpec as P

ROWS = 16
COLS = 64
WIN = 20
EDGE = 8
MESH = pl.DeviceIdType.MESH
SLOT_A = 4
SLOT_S = 8
SLOT_X = 16
SLOT_H = 8
LATER = 6


def shift_down(v, edge):
    rolled = pltpu.roll(v, 1, axis=0)
    pos = lax.broadcasted_iota(jnp.int32, v.shape, 0) % COLS
    return jnp.where(pos == 0, edge, rolled)


def shift_up(v, edge):
    rolled = pltpu.roll(v, v.shape[0] - 1, axis=0)
    pos = lax.broadcasted_iota(jnp.int32, v.shape, 0) % COLS
    return jnp.where(pos == COLS - 1, edge, rolled)


def build_x3(is_left, xc, hx, x3, xh):
    for half in range(2):
        lane = half * 128
        for r in range(WIN):
            mid = xc[half, 2 + r]
            v = mid.astype(jnp.float32)
            h = hx[half, r].astype(jnp.float32)
            near = jnp.where(is_left, h[0:1], h[EDGE - 1:EDGE])
            far = jnp.where(is_left, h[1:2], h[EDGE - 2:EDGE - 1])
            own = jnp.where(is_left, v[COLS - 1:COLS], v[0:1])
            zero = jnp.zeros_like(near)
            rows = pl.ds(r * COLS, COLS)
            x3[rows, lane:lane + 128] = shift_down(v, jnp.where(is_left, zero, near)).astype(jnp.bfloat16)
            x3[rows, 256 + lane:384 + lane] = mid
            x3[rows, 512 + lane:640 + lane] = shift_up(v, jnp.where(is_left, near, zero)).astype(jnp.bfloat16)
            xh[r:r + 1, lane:lane + 128] = jnp.where(is_left, own, far)
            xh[r:r + 1, 256 + lane:384 + lane] = near
            xh[r:r + 1, 512 + lane:640 + lane] = jnp.where(is_left, far, own)


def conv1(is_left, top, bottom, x3, xh, w1, b1, y3, blocks=((0, 10), (10, 8))):
    edge_all = None
    for first, count in blocks:
        m = count * COLS
        lhs = jnp.concatenate([x3[(first + dy) * COLS:(first + dy) * COLS + m, :] for dy in range(3)], axis=1)
        if first == 0:
            edge = jnp.concatenate([xh[dy:dy + 32, :] for dy in range(3)], axis=1).astype(jnp.bfloat16)
            lhs = jnp.concatenate([edge, lhs], axis=0)
        z = jnp.dot(lhs, w1[...].reshape(2304, 512), preferred_element_type=jnp.float32)
        z = jnp.maximum(z + b1[...], 0.0)
        if first == 0:
            edge_all = z[:32]
            z = z[32:]
        for r in range(count):
            row = first + r
            v = z[r * COLS:(r + 1) * COLS]
            e = edge_all[row:row + 1]
            if row == 0:
                v = jnp.where(top, 0.0, v)
                e = jnp.where(top, 0.0, e)
            if row == ROWS + 1:
                v = jnp.where(bottom, 0.0, v)
                e = jnp.where(bottom, 0.0, e)
            zero = jnp.zeros_like(e)
            dst = pl.ds(row * COLS, COLS)
            y3[dst, 0:512] = shift_down(v, jnp.where(is_left, zero, e)).astype(jnp.bfloat16)
            y3[dst, 512:1024] = v.astype(jnp.bfloat16)
            y3[dst, 1024:1536] = shift_up(v, jnp.where(is_left, e, zero)).astype(jnp.bfloat16)


def conv2(y3, w2, b2, out, blk=8):
    for first in range(0, ROWS, blk):
        m = blk * COLS
        lhs = jnp.concatenate([y3[(first + dy) * COLS:(first + dy) * COLS + m, :] for dy in range(3)], axis=1)
        out[first * COLS:first * COLS + m, :] = jnp.dot(lhs, w2[...], preferred_element_type=jnp.float32) + b2[...]


def merge(slot, chip, off, ab, xc_slot, sb_slot):
    for r in range(WIN):
        xc_slot[chip, off + r] = jnp.concatenate([ab[slot, 0, 0, r], ab[slot, 0, 1, r]], axis=-1)
        sb_slot[r] = jnp.concatenate([ab[slot, 1, 0, r], ab[slot, 1, 1, r]], axis=-1)


def fused_kernel(images, x, w1, b1, w2, b2, y, x_rest, h_rest, w1_all, ab, sb, xc, hx, x3, xh, y3, ob, w1v, w2v,
                 loc_sem, a_send, a_recv, x_send, x_recv, h_send, h_recv, o_sem, w_loc, w_send, w_recv, rest_sem,
                 credit_a, credit_x, credit_h):
    now = images - LATER
    data = lax.axis_index('data')
    side = lax.axis_index('cols')
    model = lax.axis_index('model')
    is_left = side == 0
    chip = model // 2
    core = model % 2
    mate = chip * 2 + 1 - core
    far = (1 - chip) * 2 + core
    far_mate = (1 - chip) * 2 + 1 - core
    to_mate = (data, side, mate)
    to_far = (data, side, far)
    to_side = (data, 1 - side, model)

    def source(m):
        return jnp.where(m == 0, 0, jnp.where(m == 3, 44, ROWS * m - 2))

    def place(m):
        return jnp.where(m == 0, 4, jnp.where(m == 3, 0, 2))

    edge = pl.multiple_of(jnp.where(is_left, COLS - EDGE, 0), EDGE)

    for slot in range(SLOT_X):
        for half in range(2):
            for row in (2, 3, 20, 21):
                xc[slot, half, row] = jnp.zeros((COLS, 128), jnp.bfloat16)
    xh[...] = jnp.zeros_like(xh)

    barrier = pltpu.get_barrier_semaphore()
    for peer in (to_mate, to_far, to_side):
        pl.semaphore_signal(barrier, inc=1, device_id=peer, device_id_type=MESH)
    pl.semaphore_wait(barrier, 3)

    def remote(src, dst, send, recv, peer):
        return pltpu.make_async_remote_copy(src_ref=src, dst_ref=dst, send_sem=send, recv_sem=recv, device_id=peer, device_id_type=MESH)

    def w1_part(m):
        return w1v.at[:, pl.ds(pl.multiple_of(m * 64, 64), 64), :]

    def w1_half(m, half):
        return w1v.at[:, pl.ds(pl.multiple_of(m * 64, 64), 64), pl.ds(pl.multiple_of(half * 256, 256), 256)]

    w_far = remote(w1.at[:, :, pl.ds(pl.multiple_of(side * 256, 256), 256)], w1_half(model, side), w_send.at[0], w_recv.at[0], to_far)
    w_side = remote(w1_half(far, side), w1_half(far, side), w_send.at[3], w_recv.at[3], to_side)
    w_pass = [remote(w1_half(far, half), w1_half(far, half), w_send.at[2 + 2 * t], w_recv.at[2 + 2 * t], to_mate)
              for t, half in enumerate((side, 1 - side))]
    w_mate = remote(w1, w1_part(model), w_send.at[1], w_recv.at[1], to_mate)
    w_own = pltpu.make_async_copy(w1, w1_part(model), w_loc.at[0])
    w2_own = pltpu.make_async_copy(w2, w2v, w_loc.at[1])

    def own_copy(n, win):
        slot = n % SLOT_A
        rows = pl.ds(source(model if win == 0 else far), WIN)
        return pltpu.make_async_copy(x.at[n, rows], ab.at[slot, win, core], loc_sem.at[slot, win])

    def mate_copy(n, win):
        slot = n % SLOT_A
        rows = pl.ds(source(mate if win == 0 else far_mate), WIN)
        return remote(x.at[n, rows], ab.at[slot, win, core], a_send.at[slot, win], a_recv.at[slot, win], to_mate)

    def is_edge(m):
        return jnp.logical_or(m == 0, m == 3)

    def by_size(m, run):
        @pl.when(is_edge(m))
        def _():
            run(WIN - 2, jnp.where(m == 3, 2, 0))

        @pl.when(jnp.logical_not(is_edge(m)))
        def _():
            run(WIN, 0)

    def far_copy(n, m, half, count, first):
        slot = n % SLOT_X
        return remote(sb.at[n % SLOT_S, pl.ds(first, count)], xc.at[slot, half, pl.ds(place(m) + first, count)],
                      x_send.at[slot], x_recv.at[slot], to_far)

    def side_copy(n):
        slot = n % SLOT_H
        return remote(xc.at[n % SLOT_X, :, pl.ds(2, WIN), pl.ds(edge, EDGE), :], hx.at[slot], h_send.at[slot], h_recv.at[slot], to_side)

    def out_copy(n):
        return pltpu.make_async_copy(ob.at[n % 2], y.at[n], o_sem.at[n % 2])

    def rest_copy(n, part):
        if part == 0:
            return pltpu.make_async_copy(xc.at[n % SLOT_X, :, pl.ds(2, WIN)], x_rest.at[n - now], rest_sem.at[n - now, 0])
        return pltpu.make_async_copy(hx.at[n % SLOT_H], h_rest.at[n - now], rest_sem.at[n - now, 1])

    def last(i):
        return jnp.clip(i + 6 + jnp.maximum(i, 0) // 4, -1, images - 1)

    def each(i, run):
        lo, hi = last(i - 1), last(i)

        @pl.when(hi > lo)
        def _():
            run(lo + 1)

        @pl.when(hi > lo + 1)
        def _():
            run(lo + 2)

    def start_a(n):
        @pl.when(n >= SLOT_A)
        def _():
            pl.semaphore_wait(credit_a, 1)
        for win in range(2):
            own_copy(n, win).start()
            mate_copy(n, win).start()

    def start_x(n):
        @pl.when(n >= SLOT_X)
        def _():
            pl.semaphore_wait(credit_x, 1)
        by_size(far, lambda count, first: far_copy(n, far, chip, count, first).start())

    def wait_a(n):
        for win in range(2):
            own_copy(n, win).wait()
            mate_copy(n, win).wait()

    def start_h(n):
        by_size(far, lambda count, first: far_copy(n, far, chip, count, first).wait_send())
        by_size(model, lambda count, first: far_copy(n, model, 1 - chip, count, first).wait_recv())

        @pl.when(n >= SLOT_H)
        def _():
            pl.semaphore_wait(credit_h, 1)
        side_copy(n).start()

    def wait_h(n):
        side_copy(n).wait()

        @pl.when(n >= now)
        def _():
            rest_copy(n, 0).start()
            rest_copy(n, 1).start()

    def control(i):
        each(i, start_a)
        each(i - 2, start_x)
        each(i - 1, wait_a)

        @pl.when(last(i - 1) > last(i - 2) + 1)
        def _():
            do_merge(last(i - 1) - 1, True)
        each(i - 4, start_h)
        each(i - 5, wait_h)

    def release(i):
        def free_a(n):
            @pl.when(n < images - SLOT_A)
            def _():
                pl.semaphore_signal(credit_a, inc=1, device_id=to_mate, device_id_type=MESH)
        each(i - 1, free_a)
        built = i + 1

        @pl.when(jnp.logical_and(built >= 0, built < images - SLOT_X))
        def _():
            pl.semaphore_signal(credit_x, inc=1, device_id=to_far, device_id_type=MESH)

        @pl.when(jnp.logical_and(built >= 0, built < images - SLOT_H))
        def _():
            pl.semaphore_signal(credit_h, inc=1, device_id=to_side, device_id_type=MESH)

    def do_merge(n, live):
        merge(n % SLOT_A, chip, place(model), ab, xc.at[jnp.where(live, n % SLOT_X, SLOT_X)], sb.at[jnp.where(live, n % SLOT_S, SLOT_S)])

    def do_build(n):
        build_x3(is_left, xc.at[n % SLOT_X], hx.at[n % SLOT_H], x3, xh)

    w_far.start()
    w_mate.start()
    w_own.start()
    w2_own.start()

    def fill(t, _):
        i = t - 6

        @pl.when(i == -2)
        def _():
            w_far.wait()
            w_side.start()
            w_pass[0].start()

        @pl.when(i == -1)
        def _():
            w_side.wait()
            w_pass[1].start()
        control(i)

        @pl.when(last(i - 1) > last(i - 2))
        def _():
            do_merge(last(i - 1), True)

        @pl.when(i + 1 >= 0)
        def _():
            do_build(i + 1)
        release(i)
        return 0

    lax.fori_loop(0, 6, fill, 0)
    w_mate.wait()
    w_own.wait()
    w2_own.wait()
    for copy in w_pass:
        copy.wait()
    w_out = pltpu.make_async_copy(w1v, w1_all, w_loc.at[2])
    w_out.start()

    def step(i, _):
        control(i)

        @pl.when(i >= 2)
        def _():
            out_copy(i - 2).wait()
        conv1(is_left, model == 0, model == 3, x3, xh, w1v, b1, y3)
        do_build(i + 1)
        do_merge(last(i - 1), last(i - 1) > last(i - 2))
        conv2(y3, w2v, b2, ob.at[i % 2])
        out_copy(i).start()
        release(i)
        return 0

    lax.fori_loop(0, now, step, 0)
    out_copy(now - 2).wait()
    out_copy(now - 1).wait()
    w_out.wait()
    for n in range(now, images):
        rest_copy(n, 0).wait()
        rest_copy(n, 1).wait()


def rest_kernel(images, y_done, x_rest, h_rest, w1, b1, w2, b2, y, xc, hx, x3, xh, y3, ob, w1v, w2v, cb,
                l_sem, w_sem, o_sem, in_sem, out_sem):
    done = images - LATER
    sets = LATER - 1
    size = -(-done // sets)
    model = lax.axis_index('model')
    is_left = lax.axis_index('cols') == 0
    weights = [pltpu.make_async_copy(w1, w1v, w_sem.at[0]), pltpu.make_async_copy(w2, w2v, w_sem.at[1])]
    xh[...] = jnp.zeros_like(xh)

    def load(n):
        return [pltpu.make_async_copy(x_rest.at[n], xc.at[n, :, pl.ds(2, WIN)], l_sem.at[n, 0]),
                pltpu.make_async_copy(h_rest.at[n], hx.at[n], l_sem.at[n, 1])]

    def bring(s, q):
        return pltpu.make_async_copy(y_done.at[s + sets * q], cb.at[s % 2, q], in_sem.at[s % 2, q])

    def put(s, q):
        return pltpu.make_async_copy(cb.at[s % 2, q], y.at[s + sets * q], out_sem.at[s % 2, q])

    def each(s, run):
        for q in range(size):
            @pl.when(jnp.logical_and(jnp.logical_and(s >= 0, s < sets), s + sets * q < done))
            def _():
                run(s, q)

    def out_copy(n):
        return pltpu.make_async_copy(ob.at[n % 2], y.at[done + n], o_sem.at[n % 2])

    for copy in load(0) + weights[:1] + load(1) + weights[1:] + [c for n in range(2, LATER) for c in load(n)]:
        copy.start()
    for copy in load(0):
        copy.wait()
    build_x3(is_left, xc.at[0], hx.at[0], x3, xh)
    for copy in weights + [c for n in range(1, LATER) for c in load(n)]:
        copy.wait()

    def step(i, _):
        each(i - 1, lambda s, q: bring(s, q).wait())
        each(i - 1, lambda s, q: put(s, q).start())
        each(i - 2, lambda s, q: put(s, q).wait())
        each(i, lambda s, q: bring(s, q).start())

        @pl.when(i >= 2)
        def _():
            out_copy(i - 2).wait()
        conv1(is_left, model == 0, model == 3, x3, xh, w1v, b1, y3)
        n = jnp.minimum(i + 1, LATER - 1)
        build_x3(is_left, xc.at[n], hx.at[n], x3, xh)
        conv2(y3, w2v, b2, ob.at[i % 2])
        out_copy(i).start()
        return 0

    lax.fori_loop(0, LATER, step, 0)
    each(jnp.int32(sets - 1), lambda s, q: put(s, q).wait())
    out_copy(LATER - 2).wait()
    out_copy(LATER - 1).wait()


def rest(images, y_done, x_rest, h_rest, w1, b1, w2, b2):
    hbm = pl.BlockSpec(memory_space=pl.ANY)
    vmem = pl.BlockSpec(memory_space=pltpu.VMEM)
    dma = pltpu.SemaphoreType.DMA
    bf16 = jnp.bfloat16
    size = -(-(images - LATER) // (LATER - 1))
    return pl.pallas_call(
        functools.partial(rest_kernel, images),
        out_shape=jax.ShapeDtypeStruct((images, ROWS * COLS, 512), jnp.float32),
        in_specs=[hbm, hbm, hbm, hbm, vmem, hbm, vmem],
        out_specs=hbm,
        scratch_shapes=[
            pltpu.VMEM((LATER, 2, WIN + 4, COLS, 128), bf16),
            pltpu.VMEM((LATER, 2, WIN, EDGE, 128), bf16),
            pltpu.VMEM((WIN * COLS, 768), bf16),
            pltpu.VMEM((40, 768), jnp.float32),
            pltpu.VMEM(((ROWS + 2) * COLS, 1536), bf16),
            pltpu.VMEM((2, ROWS * COLS, 512), jnp.float32),
            pltpu.VMEM((9, 256, 512), bf16),
            pltpu.VMEM((4608, 512), bf16),
            pltpu.VMEM((2, size, ROWS * COLS, 512), jnp.float32),
            dma((LATER, 2)), dma((2,)), dma((2,)), dma((2, size)), dma((2, size)),
        ],
        compiler_params=pltpu.CompilerParams(vmem_limit_bytes=62 * 1024 * 1024),
    )(y_done, x_rest, h_rest, w1, b1, w2, b2)


def fused(x, w1, b1, w2, b2):
    images = x.shape[0]
    hbm = pl.BlockSpec(memory_space=pl.ANY)
    vmem = pl.BlockSpec(memory_space=pltpu.VMEM)
    dma = pltpu.SemaphoreType.DMA
    bf16 = jnp.bfloat16
    return pl.pallas_call(
        functools.partial(fused_kernel, images),
        out_shape=[
            jax.ShapeDtypeStruct((images - LATER, ROWS * COLS, 512), jnp.float32),
            jax.ShapeDtypeStruct((LATER, 2, WIN, COLS, 128), bf16),
            jax.ShapeDtypeStruct((LATER, 2, WIN, EDGE, 128), bf16),
            jax.ShapeDtypeStruct((9, 256, 512), bf16),
        ],
        in_specs=[hbm, hbm, vmem, hbm, vmem],
        out_specs=[hbm] * 4,
        scratch_shapes=[
            pltpu.VMEM((SLOT_A, 2, 2, WIN, COLS, 64), bf16),
            pltpu.VMEM((SLOT_S + 1, WIN, COLS, 128), bf16),
            pltpu.VMEM((SLOT_X + 1, 2, WIN + 4, COLS, 128), bf16),
            pltpu.VMEM((SLOT_H, 2, WIN, EDGE, 128), bf16),
            pltpu.VMEM((WIN * COLS, 768), bf16),
            pltpu.VMEM((40, 768), jnp.float32),
            pltpu.VMEM(((ROWS + 2) * COLS, 1536), bf16),
            pltpu.VMEM((2, ROWS * COLS, 512), jnp.float32),
            pltpu.VMEM((9, 256, 512), bf16),
            pltpu.VMEM((4608, 512), bf16),
            dma((SLOT_A, 2)), dma((SLOT_A, 2)), dma((SLOT_A, 2)),
            dma((SLOT_X,)), dma((SLOT_X,)), dma((SLOT_H,)), dma((SLOT_H,)), dma((2,)),
            dma((3,)), dma((5,)), dma((5,)), dma((LATER, 2)),
            pltpu.SemaphoreType.REGULAR, pltpu.SemaphoreType.REGULAR, pltpu.SemaphoreType.REGULAR,
        ],
        compiler_params=pltpu.CompilerParams(vmem_limit_bytes=60 * 1024 * 1024, collective_id=0, has_side_effects=True),
    )(x, w1, b1, w2, b2)


def solution(mesh):
    def local_step(x, w1, b1, w2, b2):
        images = x.shape[0]
        b1, w2, b2 = b1.reshape(1, 512), w2.reshape(4608, 512), b2.reshape(1, 512)
        done, x_rest, h_rest, w1_all = fused(x, w1.reshape(9, 64, 512), b1, w2, b2)
        y = rest(images, done, x_rest, h_rest, w1_all, b1, w2, b2)
        return y.reshape(images, ROWS, COLS, 512)

    return jax.shard_map(local_step, mesh=mesh, in_specs=(P('data', None, 'cols', 'model'), P(None, None, 'model', None), P(), P(), P()), out_specs=P('data', 'model', 'cols', None), check_vma=False)
```

```python
import functools

import jax
import jax.numpy as jnp
from jax import lax
from jax.experimental import pallas as pl
from jax.experimental.pallas import tpu as pltpu
from jax.sharding import PartitionSpec as P

ROWS = 16
COLS = 64
WIN = 20
EDGE = 8
MESH = pl.DeviceIdType.MESH
SLOT_A = 4
SLOT_S = 10
SLOT_X = 12
SLOT_H = 8
LATER = 6
EARLY = 10
HALO = 32


def shift_down(v, edge):
    rolled = pltpu.roll(v, 1, axis=0)
    pos = lax.broadcasted_iota(jnp.int32, v.shape, 0) % COLS
    return jnp.where(pos == 0, edge, rolled)


def shift_up(v, edge):
    rolled = pltpu.roll(v, v.shape[0] - 1, axis=0)
    pos = lax.broadcasted_iota(jnp.int32, v.shape, 0) % COLS
    return jnp.where(pos == COLS - 1, edge, rolled)


def build_half(is_left, xc, hx, x3, xh):
    for r in range(WIN):
        mid = xc[2 + r]
        v = mid.astype(jnp.float32)
        h = hx[r].astype(jnp.float32)
        near = jnp.where(is_left, h[0:1], h[EDGE - 1:EDGE])
        far = jnp.where(is_left, h[1:2], h[EDGE - 2:EDGE - 1])
        own = jnp.where(is_left, v[COLS - 1:COLS], v[0:1])
        zero = jnp.zeros_like(near)
        rows = pl.ds(r * COLS, COLS)
        x3[rows, 0:128] = shift_down(v, jnp.where(is_left, zero, near)).astype(jnp.bfloat16)
        x3[rows, 128:256] = mid
        x3[rows, 256:384] = shift_up(v, jnp.where(is_left, near, zero)).astype(jnp.bfloat16)
        xh[r:r + 1, 0:128] = jnp.where(is_left, own, far)
        xh[r:r + 1, 128:256] = near
        xh[r:r + 1, 256:384] = jnp.where(is_left, far, own)


def build_x3(is_left, xc, hx, x3, xh):
    for half in range(2):
        build_half(is_left, xc.at[half], hx.at[half], x3.at[half], xh.at[half])


BLOCKS = ((0, 10), (10, 8))


def lhs_rows(x3s, xhs, first, count):
    m = count * COLS
    lhs = jnp.concatenate([x3[(first + dy) * COLS:(first + dy) * COLS + m, :] for x3 in x3s for dy in range(3)], axis=1)
    if first == 0:
        edge = jnp.concatenate([xh[dy:dy + HALO, :] for xh in xhs for dy in range(3)], axis=1).astype(jnp.bfloat16)
        lhs = jnp.concatenate([edge, lhs], axis=0)
    return lhs


def part_rows(first, count):
    start = 0 if first == 0 else HALO + first * COLS
    return slice(start, HALO + (first + count) * COLS)


def conv1_part(x3, xh, w, zp):
    for first, count in BLOCKS:
        z = jnp.dot(lhs_rows([x3], [xh], first, count), w[...].reshape(1152, 512), preferred_element_type=jnp.float32)
        zp[part_rows(first, count), :] = z.astype(jnp.bfloat16)


def conv1(is_left, top, bottom, x3s, xhs, w, depth, b1, y3, zp=None):
    edge_all = None
    for first, count in BLOCKS:
        z = jnp.dot(lhs_rows(x3s, xhs, first, count), w[...].reshape(depth, 512), preferred_element_type=jnp.float32)
        if zp is not None:
            z = z + zp[part_rows(first, count), :].astype(jnp.float32)
        z = jnp.maximum(z + b1[...], 0.0)
        if first == 0:
            edge_all = z[:HALO]
            z = z[HALO:]
        for r in range(count):
            row = first + r
            v = z[r * COLS:(r + 1) * COLS]
            e = edge_all[row:row + 1]
            if row == 0:
                v = jnp.where(top, 0.0, v)
                e = jnp.where(top, 0.0, e)
            if row == ROWS + 1:
                v = jnp.where(bottom, 0.0, v)
                e = jnp.where(bottom, 0.0, e)
            zero = jnp.zeros_like(e)
            dst = pl.ds(row * COLS, COLS)
            y3[dst, 0:512] = shift_down(v, jnp.where(is_left, zero, e)).astype(jnp.bfloat16)
            y3[dst, 512:1024] = v.astype(jnp.bfloat16)
            y3[dst, 1024:1536] = shift_up(v, jnp.where(is_left, e, zero)).astype(jnp.bfloat16)


def conv2(y3, w2, b2, out, blk=8):
    for first in range(0, ROWS, blk):
        m = blk * COLS
        lhs = jnp.concatenate([y3[(first + dy) * COLS:(first + dy) * COLS + m, :] for dy in range(3)], axis=1)
        out[first * COLS:first * COLS + m, :] = jnp.dot(lhs, w2[...], preferred_element_type=jnp.float32) + b2[...]


def merge(slot, chip, off, ab, xc_slot, sb_slot):
    for r in range(WIN):
        xc_slot[chip, off + r] = jnp.concatenate([ab[slot, 0, 0, r], ab[slot, 0, 1, r]], axis=-1)
        sb_slot[r] = jnp.concatenate([ab[slot, 1, 0, r], ab[slot, 1, 1, r]], axis=-1)


def fused_kernel(images, x, w1, b1, w2, b2, y, x_rest, h_rest, w1_all, ab, sb, xc, hx, x3, xh, y3, ob, w1v, w2v, hp, zp,
                 loc_sem, a_send, a_recv, x_send, x_recv, h_send, h_recv, o_sem, w_loc, w_send, w_recv, rest_sem, p_send, p_recv,
                 credit_a, credit_x, credit_h):
    now = images - LATER
    data = lax.axis_index('data')
    side = lax.axis_index('cols')
    model = lax.axis_index('model')
    is_left = side == 0
    chip = model // 2
    core = model % 2
    mate = chip * 2 + 1 - core
    far = (1 - chip) * 2 + core
    far_mate = (1 - chip) * 2 + 1 - core
    to_mate = (data, side, mate)
    to_far = (data, side, far)
    to_side = (data, 1 - side, model)

    def source(m):
        return jnp.where(m == 0, 0, jnp.where(m == 3, 44, ROWS * m - 2))

    def place(m):
        return jnp.where(m == 0, 4, jnp.where(m == 3, 0, 2))

    edge = pl.multiple_of(jnp.where(is_left, COLS - EDGE, 0), EDGE)

    for slot in range(SLOT_X):
        for half in range(2):
            for row in (2, 3, 20, 21):
                xc[slot, half, row] = jnp.zeros((COLS, 128), jnp.bfloat16)
    xh[...] = jnp.zeros_like(xh)

    barrier = pltpu.get_barrier_semaphore()
    for peer in (to_mate, to_far, to_side):
        pl.semaphore_signal(barrier, inc=1, device_id=peer, device_id_type=MESH)
    pl.semaphore_wait(barrier, 3)

    def remote(src, dst, send, recv, peer):
        return pltpu.make_async_remote_copy(src_ref=src, dst_ref=dst, send_sem=send, recv_sem=recv, device_id=peer, device_id_type=MESH)

    def w1_part(m):
        return w1v.at[m // 2, :, pl.ds(pl.multiple_of(m % 2 * 64, 64), 64), :]

    def w1_half(m, half):
        return w1v.at[m // 2, :, pl.ds(pl.multiple_of(m % 2 * 64, 64), 64), pl.ds(pl.multiple_of(half * 256, 256), 256)]

    w_far = remote(w1.at[:, :, pl.ds(pl.multiple_of(side * 256, 256), 256)], w1_half(model, side), w_send.at[0], w_recv.at[0], to_far)
    w_side = remote(w1_half(far, side), w1_half(far, side), w_send.at[3], w_recv.at[3], to_side)
    w_pass = [remote(w1_half(far, half), w1_half(far, half), w_send.at[2 + 2 * t], w_recv.at[2 + 2 * t], to_mate)
              for t, half in enumerate((side, 1 - side))]
    w_mate = remote(w1, w1_part(model), w_send.at[1], w_recv.at[1], to_mate)
    w_own = pltpu.make_async_copy(w1, w1_part(model), w_loc.at[0])
    w2_own = pltpu.make_async_copy(w2, w2v, w_loc.at[1])

    def own_copy(n, win):
        slot = n % SLOT_A
        rows = pl.ds(source(model if win == 0 else far), WIN)
        return pltpu.make_async_copy(x.at[n, rows], ab.at[slot, win, core], loc_sem.at[slot, win])

    def mate_copy(n, win):
        slot = n % SLOT_A
        rows = pl.ds(source(mate if win == 0 else far_mate), WIN)
        return remote(x.at[n, rows], ab.at[slot, win, core], a_send.at[slot, win], a_recv.at[slot, win], to_mate)

    def is_edge(m):
        return jnp.logical_or(m == 0, m == 3)

    def by_size(m, run):
        @pl.when(is_edge(m))
        def _():
            run(WIN - 2, jnp.where(m == 3, 2, 0))

        @pl.when(jnp.logical_not(is_edge(m)))
        def _():
            run(WIN, 0)

    def far_copy(n, m, half, count, first):
        slot = n % SLOT_X
        return remote(sb.at[n % SLOT_S, pl.ds(first, count)], xc.at[slot, half, pl.ds(place(m) + first, count)],
                      x_send.at[slot], x_recv.at[slot], to_far)

    def side_copy(n):
        slot = n % SLOT_H
        return remote(xc.at[n % SLOT_X, :, pl.ds(2, WIN), pl.ds(edge, EDGE), :], hx.at[slot], h_send.at[slot], h_recv.at[slot], to_side)

    def out_copy(n):
        return pltpu.make_async_copy(ob.at[n % 2], y.at[n], o_sem.at[n % 2])

    def rest_copy(n, part):
        if part == 0:
            return pltpu.make_async_copy(xc.at[n % SLOT_X, :, pl.ds(2, WIN)], x_rest.at[n - now], rest_sem.at[n - now, 0])
        return pltpu.make_async_copy(hx.at[n % SLOT_H], h_rest.at[n - now], rest_sem.at[n - now, 1])

    def seen(i):
        return i + 2 + jnp.maximum(i - 9, 0) // 4

    def each(i, run):
        lo, hi = seen(i - 1), seen(i)
        run(lo + 1)

        @pl.when(hi > lo + 1)
        def _():
            run(lo + 2)

    def start_a(n):
        @pl.when(n >= SLOT_A)
        def _():
            pl.semaphore_wait(credit_a, 1)
        for win in range(2):
            own_copy(n, win).start()
            mate_copy(n, win).start()

    def start_x(n):
        @pl.when(n >= SLOT_X)
        def _():
            pl.semaphore_wait(credit_x, 1)
        by_size(far, lambda count, first: far_copy(n, far, chip, count, first).start())

    def wait_a(n):
        for win in range(2):
            own_copy(n, win).wait()
            mate_copy(n, win).wait()

    def start_h(n):
        by_size(far, lambda count, first: far_copy(n, far, chip, count, first).wait_send())
        by_size(model, lambda count, first: far_copy(n, model, 1 - chip, count, first).wait_recv())

        @pl.when(n >= SLOT_H)
        def _():
            pl.semaphore_wait(credit_h, 1)
        side_copy(n).start()

    def wait_h(n):
        side_copy(n).wait()

        @pl.when(n >= now)
        def _():
            rest_copy(n, 0).start()
            rest_copy(n, 1).start()

    def part_copy(n):
        return remote(xc.at[n % SLOT_X, chip, pl.ds(2, WIN), pl.ds(edge, EDGE), :], hp.at[n], p_send.at[n], p_recv.at[n], to_side)

    def control(i):
        @pl.when(i + EARLY + 1 < images)
        def _():
            start_a(i + EARLY + 1)

        @pl.when(jnp.logical_and(i >= 1, i + EARLY - 1 < images))
        def _():
            start_x(i + EARLY - 1)

        @pl.when(i + EARLY < images)
        def _():
            wait_a(i + EARLY)
        each(i, start_h)
        each(i - 1, wait_h)

    def free_a(n):
        @pl.when(n < images - SLOT_A)
        def _():
            pl.semaphore_signal(credit_a, inc=1, device_id=to_mate, device_id_type=MESH)

    def free_built(n):
        @pl.when(n < images - SLOT_X)
        def _():
            pl.semaphore_signal(credit_x, inc=1, device_id=to_far, device_id_type=MESH)

        @pl.when(n < images - SLOT_H)
        def _():
            pl.semaphore_signal(credit_h, inc=1, device_id=to_side, device_id_type=MESH)

    def do_merge(n, live):
        merge(n % SLOT_A, chip, place(model), ab, xc.at[jnp.where(live, n % SLOT_X, SLOT_X)], sb.at[jnp.where(live, n % SLOT_S, SLOT_S)])

    def do_build(n):
        build_x3(is_left, xc.at[n % SLOT_X], hx.at[n % SLOT_H], x3, xh)

    w_far.start()
    w_mate.start()
    w_own.start()
    w2_own.start()

    for n in range(3):
        start_a(n)
    w_own.wait()
    w_mate.wait()

    def fill(t, _):
        @pl.when(t < EARLY)
        def _():
            wait_a(t)

        @pl.when(jnp.logical_and(t >= 1, t <= EARLY))
        def _():
            start_x(t - 1)
            part_copy(t - 1).start()

        @pl.when(t + 3 <= EARLY)
        def _():
            start_a(t + 3)

        @pl.when(t < EARLY)
        def _():
            do_merge(t, True)
            free_a(t)

        @pl.when(t == 4)
        def _():
            w_far.wait()
            w_side.start()
            w_pass[0].start()

        @pl.when(t == 8)
        def _():
            w_side.wait()
            w_pass[1].start()

        @pl.when(t == 9)
        def _():
            start_h(0)

        @pl.when(t == EARLY + 1)
        def _():
            start_h(1)

        @pl.when(t >= 2)
        def _():
            n = t - 2
            part_copy(n).wait()
            build_half(is_left, xc.at[n % SLOT_X, chip], hp.at[n], x3.at[chip], xh.at[chip])
            conv1_part(x3.at[chip], xh.at[chip], w1v.at[chip], zp.at[n])
        return 0

    lax.fori_loop(0, EARLY + 2, fill, 0)
    w2_own.wait()
    for copy in w_pass:
        copy.wait()
    wait_h(0)
    do_build(0)
    free_built(0)
    w_out = pltpu.make_async_copy(w1v, w1_all, w_loc.at[2])
    w_out.start()

    def step(early, i, _):
        control(i)

        @pl.when(i >= 2)
        def _():
            out_copy(i - 2).wait()
        if early:
            conv1(is_left, model == 0, model == 3, [x3.at[1 - chip]], [xh.at[1 - chip]], w1v.at[1 - chip], 1152, b1, y3, zp.at[i])
        else:
            conv1(is_left, model == 0, model == 3, [x3.at[0], x3.at[1]], [xh.at[0], xh.at[1]], w1v, 2304, b1, y3)
        do_build(i + 1)
        do_merge(i + EARLY, i + EARLY < images)
        conv2(y3, w2v, b2, ob.at[i % 2])
        out_copy(i).start()

        @pl.when(i + EARLY < images)
        def _():
            free_a(i + EARLY)
        free_built(i + 1)
        return 0

    lax.fori_loop(0, EARLY, functools.partial(step, True), 0)
    lax.fori_loop(EARLY, now, functools.partial(step, False), 0)
    each(now - 1, wait_h)
    out_copy(now - 2).wait()
    out_copy(now - 1).wait()
    w_out.wait()
    for n in range(now, images):
        rest_copy(n, 0).wait()
        rest_copy(n, 1).wait()


def rest_kernel(images, y_done, x_rest, h_rest, w1, b1, w2, b2, y, xc, hx, x3, xh, y3, ob, w1v, w2v, cb,
                l_sem, w_sem, o_sem, in_sem, out_sem):
    done = images - LATER
    sets = LATER - 1
    size = -(-done // sets)
    model = lax.axis_index('model')
    is_left = lax.axis_index('cols') == 0
    weights = [pltpu.make_async_copy(w1, w1v, w_sem.at[0]), pltpu.make_async_copy(w2, w2v, w_sem.at[1])]
    xh[...] = jnp.zeros_like(xh)

    def load(n):
        return [pltpu.make_async_copy(x_rest.at[n], xc.at[n, :, pl.ds(2, WIN)], l_sem.at[n, 0]),
                pltpu.make_async_copy(h_rest.at[n], hx.at[n], l_sem.at[n, 1])]

    def bring(s, q):
        return pltpu.make_async_copy(y_done.at[s + sets * q], cb.at[s % 2, q], in_sem.at[s % 2, q])

    def put(s, q):
        return pltpu.make_async_copy(cb.at[s % 2, q], y.at[s + sets * q], out_sem.at[s % 2, q])

    def each(s, run):
        for q in range(size):
            @pl.when(jnp.logical_and(jnp.logical_and(s >= 0, s < sets), s + sets * q < done))
            def _():
                run(s, q)

    def out_copy(n):
        return pltpu.make_async_copy(ob.at[n % 2], y.at[done + n], o_sem.at[n % 2])

    for copy in load(0) + weights[:1] + load(1) + weights[1:] + [c for n in range(2, LATER) for c in load(n)]:
        copy.start()
    for copy in load(0):
        copy.wait()
    build_x3(is_left, xc.at[0], hx.at[0], x3, xh)
    for copy in weights + [c for n in range(1, LATER) for c in load(n)]:
        copy.wait()

    def step(i, _):
        each(i - 1, lambda s, q: bring(s, q).wait())
        each(i - 1, lambda s, q: put(s, q).start())
        each(i - 2, lambda s, q: put(s, q).wait())
        each(i, lambda s, q: bring(s, q).start())

        @pl.when(i >= 2)
        def _():
            out_copy(i - 2).wait()
        conv1(is_left, model == 0, model == 3, [x3.at[0], x3.at[1]], [xh.at[0], xh.at[1]], w1v, 2304, b1, y3)
        n = jnp.minimum(i + 1, LATER - 1)
        build_x3(is_left, xc.at[n], hx.at[n], x3, xh)
        conv2(y3, w2v, b2, ob.at[i % 2])
        out_copy(i).start()
        return 0

    lax.fori_loop(0, LATER, step, 0)
    each(jnp.int32(sets - 1), lambda s, q: put(s, q).wait())
    out_copy(LATER - 2).wait()
    out_copy(LATER - 1).wait()


def rest(images, y_done, x_rest, h_rest, w1, b1, w2, b2):
    hbm = pl.BlockSpec(memory_space=pl.ANY)
    vmem = pl.BlockSpec(memory_space=pltpu.VMEM)
    dma = pltpu.SemaphoreType.DMA
    bf16 = jnp.bfloat16
    size = -(-(images - LATER) // (LATER - 1))
    return pl.pallas_call(
        functools.partial(rest_kernel, images),
        out_shape=jax.ShapeDtypeStruct((images, ROWS * COLS, 512), jnp.float32),
        in_specs=[hbm, hbm, hbm, hbm, vmem, hbm, vmem],
        out_specs=hbm,
        scratch_shapes=[
            pltpu.VMEM((LATER, 2, WIN + 4, COLS, 128), bf16),
            pltpu.VMEM((LATER, 2, WIN, EDGE, 128), bf16),
            pltpu.VMEM((2, WIN * COLS, 384), bf16),
            pltpu.VMEM((2, 40, 384), jnp.float32),
            pltpu.VMEM(((ROWS + 2) * COLS, 1536), bf16),
            pltpu.VMEM((2, ROWS * COLS, 512), jnp.float32),
            pltpu.VMEM((2, 9, 128, 512), bf16),
            pltpu.VMEM((4608, 512), bf16),
            pltpu.VMEM((2, size, ROWS * COLS, 512), jnp.float32),
            dma((LATER, 2)), dma((2,)), dma((2,)), dma((2, size)), dma((2, size)),
        ],
        compiler_params=pltpu.CompilerParams(vmem_limit_bytes=62 * 1024 * 1024),
    )(y_done, x_rest, h_rest, w1, b1, w2, b2)


def fused(x, w1, b1, w2, b2):
    images = x.shape[0]
    hbm = pl.BlockSpec(memory_space=pl.ANY)
    vmem = pl.BlockSpec(memory_space=pltpu.VMEM)
    dma = pltpu.SemaphoreType.DMA
    bf16 = jnp.bfloat16
    return pl.pallas_call(
        functools.partial(fused_kernel, images),
        out_shape=[
            jax.ShapeDtypeStruct((images - LATER, ROWS * COLS, 512), jnp.float32),
            jax.ShapeDtypeStruct((LATER, 2, WIN, COLS, 128), bf16),
            jax.ShapeDtypeStruct((LATER, 2, WIN, EDGE, 128), bf16),
            jax.ShapeDtypeStruct((2, 9, 128, 512), bf16),
        ],
        in_specs=[hbm, hbm, vmem, hbm, vmem],
        out_specs=[hbm] * 4,
        scratch_shapes=[
            pltpu.VMEM((SLOT_A, 2, 2, WIN, COLS, 64), bf16),
            pltpu.VMEM((SLOT_S + 1, WIN, COLS, 128), bf16),
            pltpu.VMEM((SLOT_X + 1, 2, WIN + 4, COLS, 128), bf16),
            pltpu.VMEM((SLOT_H, 2, WIN, EDGE, 128), bf16),
            pltpu.VMEM((2, WIN * COLS, 384), bf16),
            pltpu.VMEM((2, 40, 384), jnp.float32),
            pltpu.VMEM(((ROWS + 2) * COLS, 1536), bf16),
            pltpu.VMEM((2, ROWS * COLS, 512), jnp.float32),
            pltpu.VMEM((2, 9, 128, 512), bf16),
            pltpu.VMEM((4608, 512), bf16),
            pltpu.VMEM((EARLY, WIN, EDGE, 128), bf16),
            pltpu.VMEM((EARLY, HALO + (ROWS + 2) * COLS, 512), bf16),
            dma((SLOT_A, 2)), dma((SLOT_A, 2)), dma((SLOT_A, 2)),
            dma((SLOT_X,)), dma((SLOT_X,)), dma((SLOT_H,)), dma((SLOT_H,)), dma((2,)),
            dma((3,)), dma((5,)), dma((5,)), dma((LATER, 2)), dma((EARLY,)), dma((EARLY,)),
            pltpu.SemaphoreType.REGULAR, pltpu.SemaphoreType.REGULAR, pltpu.SemaphoreType.REGULAR,
        ],
        compiler_params=pltpu.CompilerParams(vmem_limit_bytes=60 * 1024 * 1024, collective_id=0, has_side_effects=True),
    )(x, w1, b1, w2, b2)


def solution(mesh):
    def local_step(x, w1, b1, w2, b2):
        images = x.shape[0]
        b1, w2, b2 = b1.reshape(1, 512), w2.reshape(4608, 512), b2.reshape(1, 512)
        done, x_rest, h_rest, w1_all = fused(x, w1.reshape(9, 64, 512), b1, w2, b2)
        y = rest(images, done, x_rest, h_rest, w1_all, b1, w2, b2)
        return y.reshape(images, ROWS, COLS, 512)

    return jax.shard_map(local_step, mesh=mesh, in_specs=(P('data', None, 'cols', 'model'), P(None, None, 'model', None), P(), P(), P()), out_specs=P('data', 'model', 'cols', None), check_vma=False)
```

```python
import functools

import jax
import jax.numpy as jnp
from jax import lax
from jax.experimental import pallas as pl
from jax.experimental.pallas import tpu as pltpu
from jax.sharding import PartitionSpec as P

ROWS = 16
COLS = 64
WIN = 20
EDGE = 8
MESH = pl.DeviceIdType.MESH
SLOT_A = 4
SLOT_S = 10
SLOT_X = 12
SLOT_H = 8
LATER = 5
EARLY = 10
HALO = 32


def shift_down(v, edge):
    rolled = pltpu.roll(v, 1, axis=0)
    pos = lax.broadcasted_iota(jnp.int32, v.shape, 0) % COLS
    return jnp.where(pos == 0, edge, rolled)


def shift_up(v, edge):
    rolled = pltpu.roll(v, v.shape[0] - 1, axis=0)
    pos = lax.broadcasted_iota(jnp.int32, v.shape, 0) % COLS
    return jnp.where(pos == COLS - 1, edge, rolled)


def build_half(is_left, xc, hx, x3, xh):
    for r in range(WIN):
        mid = xc[2 + r]
        v = mid.astype(jnp.float32)
        h = hx[r].astype(jnp.float32)
        near = jnp.where(is_left, h[0:1], h[EDGE - 1:EDGE])
        far = jnp.where(is_left, h[1:2], h[EDGE - 2:EDGE - 1])
        own = jnp.where(is_left, v[COLS - 1:COLS], v[0:1])
        zero = jnp.zeros_like(near)
        rows = pl.ds(r * COLS, COLS)
        x3[rows, 0:128] = shift_down(v, jnp.where(is_left, zero, near)).astype(jnp.bfloat16)
        x3[rows, 128:256] = mid
        x3[rows, 256:384] = shift_up(v, jnp.where(is_left, near, zero)).astype(jnp.bfloat16)
        xh[r:r + 1, 0:128] = jnp.where(is_left, own, far)
        xh[r:r + 1, 128:256] = near
        xh[r:r + 1, 256:384] = jnp.where(is_left, far, own)


def build_x3(is_left, xc, hx, x3, xh):
    for half in range(2):
        build_half(is_left, xc.at[half], hx.at[half], x3.at[half], xh.at[half])


BLOCKS = ((0, 10), (10, 8))


def lhs_rows(x3s, xhs, first, count):
    m = count * COLS
    lhs = jnp.concatenate([x3[(first + dy) * COLS:(first + dy) * COLS + m, :] for x3 in x3s for dy in range(3)], axis=1)
    if first == 0:
        edge = jnp.concatenate([xh[dy:dy + HALO, :] for xh in xhs for dy in range(3)], axis=1).astype(jnp.bfloat16)
        lhs = jnp.concatenate([edge, lhs], axis=0)
    return lhs


def part_rows(first, count):
    start = 0 if first == 0 else HALO + first * COLS
    return slice(start, HALO + (first + count) * COLS)


def conv1_part(x3, xh, w, zp):
    for first, count in BLOCKS:
        z = jnp.dot(lhs_rows([x3], [xh], first, count), w[...].reshape(1152, 512), preferred_element_type=jnp.float32)
        zp[part_rows(first, count), :] = z.astype(jnp.bfloat16)


def conv1(is_left, top, bottom, x3s, xhs, w, depth, b1, y3, zp=None):
    edge_all = None
    for first, count in BLOCKS:
        z = jnp.dot(lhs_rows(x3s, xhs, first, count), w[...].reshape(depth, 512), preferred_element_type=jnp.float32)
        if zp is not None:
            z = z + zp[part_rows(first, count), :].astype(jnp.float32)
        z = jnp.maximum(z + b1[...], 0.0)
        if first == 0:
            edge_all = z[:HALO]
            z = z[HALO:]
        for r in range(count):
            row = first + r
            v = z[r * COLS:(r + 1) * COLS]
            e = edge_all[row:row + 1]
            if row == 0:
                v = jnp.where(top, 0.0, v)
                e = jnp.where(top, 0.0, e)
            if row == ROWS + 1:
                v = jnp.where(bottom, 0.0, v)
                e = jnp.where(bottom, 0.0, e)
            zero = jnp.zeros_like(e)
            dst = pl.ds(row * COLS, COLS)
            y3[dst, 0:512] = shift_down(v, jnp.where(is_left, zero, e)).astype(jnp.bfloat16)
            y3[dst, 512:1024] = v.astype(jnp.bfloat16)
            y3[dst, 1024:1536] = shift_up(v, jnp.where(is_left, e, zero)).astype(jnp.bfloat16)


def conv2(y3, w2, b2, out, blk=8):
    for first in range(0, ROWS, blk):
        m = blk * COLS
        lhs = jnp.concatenate([y3[(first + dy) * COLS:(first + dy) * COLS + m, :] for dy in range(3)], axis=1)
        out[first * COLS:first * COLS + m, :] = jnp.dot(lhs, w2[...], preferred_element_type=jnp.float32) + b2[...]


def merge(slot, chip, off, ab, xc_slot, sb_slot):
    for r in range(WIN):
        xc_slot[chip, off + r] = jnp.concatenate([ab[slot, 0, 0, r], ab[slot, 0, 1, r]], axis=-1)
        sb_slot[r] = jnp.concatenate([ab[slot, 1, 0, r], ab[slot, 1, 1, r]], axis=-1)


def fused_kernel(images, x, w1, b1, w2, b2, y, x_rest, h_rest, w1_all, ab, sb, xc, hx, x3, xh, y3, ob, w1v, w2v, hp, zp,
                 loc_sem, a_send, a_recv, x_send, x_recv, h_send, h_recv, o_sem, w_loc, w_send, w_recv, rest_sem, p_send, p_recv,
                 credit_a, credit_x, credit_h):
    now = images - LATER
    data = lax.axis_index('data')
    side = lax.axis_index('cols')
    model = lax.axis_index('model')
    is_left = side == 0
    chip = model // 2
    core = model % 2
    mate = chip * 2 + 1 - core
    far = (1 - chip) * 2 + core
    far_mate = (1 - chip) * 2 + 1 - core
    to_mate = (data, side, mate)
    to_far = (data, side, far)
    to_side = (data, 1 - side, model)

    def source(m):
        return jnp.where(m == 0, 0, jnp.where(m == 3, 44, ROWS * m - 2))

    def place(m):
        return jnp.where(m == 0, 4, jnp.where(m == 3, 0, 2))

    edge = pl.multiple_of(jnp.where(is_left, COLS - EDGE, 0), EDGE)

    for slot in range(SLOT_X):
        for half in range(2):
            for row in (2, 3, 20, 21):
                xc[slot, half, row] = jnp.zeros((COLS, 128), jnp.bfloat16)
    xh[...] = jnp.zeros_like(xh)

    barrier = pltpu.get_barrier_semaphore()
    for peer in (to_mate, to_far, to_side):
        pl.semaphore_signal(barrier, inc=1, device_id=peer, device_id_type=MESH)
    pl.semaphore_wait(barrier, 3)

    def remote(src, dst, send, recv, peer):
        return pltpu.make_async_remote_copy(src_ref=src, dst_ref=dst, send_sem=send, recv_sem=recv, device_id=peer, device_id_type=MESH)

    def w1_part(m):
        return w1v.at[m // 2, :, pl.ds(pl.multiple_of(m % 2 * 64, 64), 64), :]

    def w1_half(m, half):
        return w1v.at[m // 2, :, pl.ds(pl.multiple_of(m % 2 * 64, 64), 64), pl.ds(pl.multiple_of(half * 256, 256), 256)]

    w_far = remote(w1.at[:, :, pl.ds(pl.multiple_of(side * 256, 256), 256)], w1_half(model, side), w_send.at[0], w_recv.at[0], to_far)
    w_side = remote(w1_half(far, side), w1_half(far, side), w_send.at[3], w_recv.at[3], to_side)
    w_pass = [remote(w1_half(far, half), w1_half(far, half), w_send.at[2 + 2 * t], w_recv.at[2 + 2 * t], to_mate)
              for t, half in enumerate((side, 1 - side))]
    w_mate = remote(w1, w1_part(model), w_send.at[1], w_recv.at[1], to_mate)
    w_own = pltpu.make_async_copy(w1, w1_part(model), w_loc.at[0])
    w2_own = pltpu.make_async_copy(w2, w2v, w_loc.at[1])

    def own_copy(n, win):
        slot = n % SLOT_A
        rows = pl.ds(source(model if win == 0 else far), WIN)
        return pltpu.make_async_copy(x.at[n, rows], ab.at[slot, win, core], loc_sem.at[slot, win])

    def mate_copy(n, win):
        slot = n % SLOT_A
        rows = pl.ds(source(mate if win == 0 else far_mate), WIN)
        return remote(x.at[n, rows], ab.at[slot, win, core], a_send.at[slot, win], a_recv.at[slot, win], to_mate)

    def is_edge(m):
        return jnp.logical_or(m == 0, m == 3)

    def by_size(m, run):
        @pl.when(is_edge(m))
        def _():
            run(WIN - 2, jnp.where(m == 3, 2, 0))

        @pl.when(jnp.logical_not(is_edge(m)))
        def _():
            run(WIN, 0)

    def far_copy(n, m, half, count, first):
        slot = n % SLOT_X
        return remote(sb.at[n % SLOT_S, pl.ds(first, count)], xc.at[slot, half, pl.ds(place(m) + first, count)],
                      x_send.at[slot], x_recv.at[slot], to_far)

    def side_copy(n):
        slot = n % SLOT_H
        return remote(xc.at[n % SLOT_X, :, pl.ds(2, WIN), pl.ds(edge, EDGE), :], hx.at[slot], h_send.at[slot], h_recv.at[slot], to_side)

    def out_copy(n):
        return pltpu.make_async_copy(ob.at[n % 2], y.at[n], o_sem.at[n % 2])

    def rest_copy(n, part):
        if part == 0:
            return pltpu.make_async_copy(xc.at[n % SLOT_X, :, pl.ds(2, WIN)], x_rest.at[n - now], rest_sem.at[n - now, 0])
        return pltpu.make_async_copy(hx.at[n % SLOT_H], h_rest.at[n - now], rest_sem.at[n - now, 1])

    def seen(i):
        return i + 2 + jnp.maximum(i - 10, 0) // 8

    def each(i, run):
        lo, hi = seen(i - 1), seen(i)
        run(lo + 1)

        @pl.when(hi > lo + 1)
        def _():
            run(lo + 2)

    def start_a(n):
        @pl.when(n >= SLOT_A)
        def _():
            pl.semaphore_wait(credit_a, 1)
        for win in range(2):
            own_copy(n, win).start()
            mate_copy(n, win).start()

    def start_x(n):
        @pl.when(n >= SLOT_X)
        def _():
            pl.semaphore_wait(credit_x, 1)
        by_size(far, lambda count, first: far_copy(n, far, chip, count, first).start())

    def wait_a(n):
        for win in range(2):
            own_copy(n, win).wait()
            mate_copy(n, win).wait()

    def start_h(n):
        by_size(far, lambda count, first: far_copy(n, far, chip, count, first).wait_send())
        by_size(model, lambda count, first: far_copy(n, model, 1 - chip, count, first).wait_recv())

        @pl.when(n >= SLOT_H)
        def _():
            pl.semaphore_wait(credit_h, 1)
        side_copy(n).start()

    def wait_h(n):
        side_copy(n).wait()

        @pl.when(n >= now)
        def _():
            rest_copy(n, 0).start()
            rest_copy(n, 1).start()

    def part_copy(n):
        return remote(xc.at[n % SLOT_X, chip, pl.ds(2, WIN), pl.ds(edge, EDGE), :], hp.at[n], p_send.at[n], p_recv.at[n], to_side)

    def control(i):
        @pl.when(i + EARLY + 1 < images)
        def _():
            start_a(i + EARLY + 1)

        @pl.when(jnp.logical_and(i >= 1, i + EARLY - 1 < images))
        def _():
            start_x(i + EARLY - 1)

        @pl.when(i + EARLY < images)
        def _():
            wait_a(i + EARLY)
        each(i, start_h)
        each(i - 1, wait_h)

    def free_a(n):
        @pl.when(n < images - SLOT_A)
        def _():
            pl.semaphore_signal(credit_a, inc=1, device_id=to_mate, device_id_type=MESH)

    def free_built(n):
        @pl.when(n < images - SLOT_X)
        def _():
            pl.semaphore_signal(credit_x, inc=1, device_id=to_far, device_id_type=MESH)

        @pl.when(n < images - SLOT_H)
        def _():
            pl.semaphore_signal(credit_h, inc=1, device_id=to_side, device_id_type=MESH)

    def do_merge(n, live):
        merge(n % SLOT_A, chip, place(model), ab, xc.at[jnp.where(live, n % SLOT_X, SLOT_X)], sb.at[jnp.where(live, n % SLOT_S, SLOT_S)])

    def do_build(n):
        build_x3(is_left, xc.at[n % SLOT_X], hx.at[n % SLOT_H], x3, xh)

    w_far.start()
    w_mate.start()
    w_own.start()
    w2_own.start()

    for n in range(3):
        start_a(n)
    w_own.wait()
    w_mate.wait()

    def fill(t, _):
        @pl.when(t < EARLY)
        def _():
            wait_a(t)

        @pl.when(jnp.logical_and(t >= 1, t <= EARLY))
        def _():
            start_x(t - 1)
            part_copy(t - 1).start()

        @pl.when(t + 3 <= EARLY)
        def _():
            start_a(t + 3)

        @pl.when(t < EARLY)
        def _():
            do_merge(t, True)
            free_a(t)

        @pl.when(t == 4)
        def _():
            w_far.wait()
            w_side.start()
            w_pass[0].start()

        @pl.when(t == 8)
        def _():
            w_side.wait()
            w_pass[1].start()

        @pl.when(t == 9)
        def _():
            start_h(0)

        @pl.when(t == EARLY + 1)
        def _():
            start_h(1)

        @pl.when(t >= 2)
        def _():
            n = t - 2
            part_copy(n).wait()
            build_half(is_left, xc.at[n % SLOT_X, chip], hp.at[n], x3.at[chip], xh.at[chip])
            conv1_part(x3.at[chip], xh.at[chip], w1v.at[chip], zp.at[n])
        return 0

    lax.fori_loop(0, EARLY + 2, fill, 0)
    w2_own.wait()
    for copy in w_pass:
        copy.wait()
    wait_h(0)
    do_build(0)
    free_built(0)
    w_out = pltpu.make_async_copy(w1v, w1_all, w_loc.at[2])
    w_out.start()

    def step(early, i, _):
        control(i)

        @pl.when(i >= 2)
        def _():
            out_copy(i - 2).wait()
        if early:
            conv1(is_left, model == 0, model == 3, [x3.at[1 - chip]], [xh.at[1 - chip]], w1v.at[1 - chip], 1152, b1, y3, zp.at[i])
        else:
            conv1(is_left, model == 0, model == 3, [x3.at[0], x3.at[1]], [xh.at[0], xh.at[1]], w1v, 2304, b1, y3)
        do_build(i + 1)
        do_merge(i + EARLY, i + EARLY < images)
        conv2(y3, w2v, b2, ob.at[i % 2])
        out_copy(i).start()

        @pl.when(i + EARLY < images)
        def _():
            free_a(i + EARLY)
        free_built(i + 1)
        return 0

    lax.fori_loop(0, EARLY, functools.partial(step, True), 0)
    lax.fori_loop(EARLY, now, functools.partial(step, False), 0)
    late = images - 1
    start_h(late)
    each(now - 1, wait_h)
    wait_h(late)
    out_copy(now - 2).wait()
    out_copy(now - 1).wait()
    w_out.wait()
    for n in range(now, images):
        rest_copy(n, 0).wait()
        rest_copy(n, 1).wait()


def rest_kernel(images, y_done, x_rest, h_rest, w1, b1, w2, b2, y, xc, hx, x3, xh, y3, ob, w1v, w2v, cb,
                l_sem, w_sem, o_sem, in_sem, out_sem):
    done = images - LATER
    sets = LATER - 1
    size = -(-done // sets)
    model = lax.axis_index('model')
    is_left = lax.axis_index('cols') == 0
    weights = [pltpu.make_async_copy(w1, w1v, w_sem.at[0]), pltpu.make_async_copy(w2, w2v, w_sem.at[1])]
    xh[...] = jnp.zeros_like(xh)

    def load(n):
        return [pltpu.make_async_copy(x_rest.at[n], xc.at[n, :, pl.ds(2, WIN)], l_sem.at[n, 0]),
                pltpu.make_async_copy(h_rest.at[n], hx.at[n], l_sem.at[n, 1])]

    def bring(s, q):
        return pltpu.make_async_copy(y_done.at[s + sets * q], cb.at[s % 2, q], in_sem.at[s % 2, q])

    def put(s, q):
        return pltpu.make_async_copy(cb.at[s % 2, q], y.at[s + sets * q], out_sem.at[s % 2, q])

    def each(s, run):
        for q in range(size):
            @pl.when(jnp.logical_and(jnp.logical_and(s >= 0, s < sets), s + sets * q < done))
            def _():
                run(s, q)

    def out_copy(n):
        return pltpu.make_async_copy(ob.at[n % 2], y.at[done + n], o_sem.at[n % 2])

    for copy in load(0) + weights[:1] + load(1) + weights[1:] + [c for n in range(2, LATER) for c in load(n)]:
        copy.start()
    for copy in load(0):
        copy.wait()
    build_x3(is_left, xc.at[0], hx.at[0], x3, xh)
    for copy in weights + [c for n in range(1, LATER) for c in load(n)]:
        copy.wait()

    def step(i, _):
        each(i - 1, lambda s, q: bring(s, q).wait())
        each(i - 1, lambda s, q: put(s, q).start())
        each(i - 2, lambda s, q: put(s, q).wait())
        each(i, lambda s, q: bring(s, q).start())

        @pl.when(i >= 2)
        def _():
            out_copy(i - 2).wait()
        conv1(is_left, model == 0, model == 3, [x3.at[0], x3.at[1]], [xh.at[0], xh.at[1]], w1v, 2304, b1, y3)
        n = jnp.minimum(i + 1, LATER - 1)
        build_x3(is_left, xc.at[n], hx.at[n], x3, xh)
        conv2(y3, w2v, b2, ob.at[i % 2])
        out_copy(i).start()
        return 0

    lax.fori_loop(0, LATER, step, 0)
    each(jnp.int32(sets - 1), lambda s, q: put(s, q).wait())
    out_copy(LATER - 2).wait()
    out_copy(LATER - 1).wait()


def rest(images, y_done, x_rest, h_rest, w1, b1, w2, b2):
    hbm = pl.BlockSpec(memory_space=pl.ANY)
    vmem = pl.BlockSpec(memory_space=pltpu.VMEM)
    dma = pltpu.SemaphoreType.DMA
    bf16 = jnp.bfloat16
    size = -(-(images - LATER) // (LATER - 1))
    return pl.pallas_call(
        functools.partial(rest_kernel, images),
        out_shape=jax.ShapeDtypeStruct((images, ROWS * COLS, 512), jnp.float32),
        in_specs=[hbm, hbm, hbm, hbm, vmem, hbm, vmem],
        out_specs=hbm,
        scratch_shapes=[
            pltpu.VMEM((LATER, 2, WIN + 4, COLS, 128), bf16),
            pltpu.VMEM((LATER, 2, WIN, EDGE, 128), bf16),
            pltpu.VMEM((2, WIN * COLS, 384), bf16),
            pltpu.VMEM((2, 40, 384), jnp.float32),
            pltpu.VMEM(((ROWS + 2) * COLS, 1536), bf16),
            pltpu.VMEM((2, ROWS * COLS, 512), jnp.float32),
            pltpu.VMEM((2, 9, 128, 512), bf16),
            pltpu.VMEM((4608, 512), bf16),
            pltpu.VMEM((2, size, ROWS * COLS, 512), jnp.float32),
            dma((LATER, 2)), dma((2,)), dma((2,)), dma((2, size)), dma((2, size)),
        ],
        compiler_params=pltpu.CompilerParams(vmem_limit_bytes=62 * 1024 * 1024),
    )(y_done, x_rest, h_rest, w1, b1, w2, b2)


def fused(x, w1, b1, w2, b2):
    images = x.shape[0]
    hbm = pl.BlockSpec(memory_space=pl.ANY)
    vmem = pl.BlockSpec(memory_space=pltpu.VMEM)
    dma = pltpu.SemaphoreType.DMA
    bf16 = jnp.bfloat16
    return pl.pallas_call(
        functools.partial(fused_kernel, images),
        out_shape=[
            jax.ShapeDtypeStruct((images - LATER, ROWS * COLS, 512), jnp.float32),
            jax.ShapeDtypeStruct((LATER, 2, WIN, COLS, 128), bf16),
            jax.ShapeDtypeStruct((LATER, 2, WIN, EDGE, 128), bf16),
            jax.ShapeDtypeStruct((2, 9, 128, 512), bf16),
        ],
        in_specs=[hbm, hbm, vmem, hbm, vmem],
        out_specs=[hbm] * 4,
        scratch_shapes=[
            pltpu.VMEM((SLOT_A, 2, 2, WIN, COLS, 64), bf16),
            pltpu.VMEM((SLOT_S + 1, WIN, COLS, 128), bf16),
            pltpu.VMEM((SLOT_X + 1, 2, WIN + 4, COLS, 128), bf16),
            pltpu.VMEM((SLOT_H, 2, WIN, EDGE, 128), bf16),
            pltpu.VMEM((2, WIN * COLS, 384), bf16),
            pltpu.VMEM((2, 40, 384), jnp.float32),
            pltpu.VMEM(((ROWS + 2) * COLS, 1536), bf16),
            pltpu.VMEM((2, ROWS * COLS, 512), jnp.float32),
            pltpu.VMEM((2, 9, 128, 512), bf16),
            pltpu.VMEM((4608, 512), bf16),
            pltpu.VMEM((EARLY, WIN, EDGE, 128), bf16),
            pltpu.VMEM((EARLY, HALO + (ROWS + 2) * COLS, 512), bf16),
            dma((SLOT_A, 2)), dma((SLOT_A, 2)), dma((SLOT_A, 2)),
            dma((SLOT_X,)), dma((SLOT_X,)), dma((SLOT_H,)), dma((SLOT_H,)), dma((2,)),
            dma((3,)), dma((5,)), dma((5,)), dma((LATER, 2)), dma((EARLY,)), dma((EARLY,)),
            pltpu.SemaphoreType.REGULAR, pltpu.SemaphoreType.REGULAR, pltpu.SemaphoreType.REGULAR,
        ],
        compiler_params=pltpu.CompilerParams(vmem_limit_bytes=60 * 1024 * 1024, collective_id=0, has_side_effects=True),
    )(x, w1, b1, w2, b2)


def solution(mesh):
    def local_step(x, w1, b1, w2, b2):
        images = x.shape[0]
        b1, w2, b2 = b1.reshape(1, 512), w2.reshape(4608, 512), b2.reshape(1, 512)
        done, x_rest, h_rest, w1_all = fused(x, w1.reshape(9, 64, 512), b1, w2, b2)
        y = rest(images, done, x_rest, h_rest, w1_all, b1, w2, b2)
        return y.reshape(images, ROWS, COLS, 512)

    return jax.shard_map(local_step, mesh=mesh, in_specs=(P('data', None, 'cols', 'model'), P(None, None, 'model', None), P(), P(), P()), out_specs=P('data', 'model', 'cols', None), check_vma=False)
```

```python
import functools

import jax
import jax.numpy as jnp
from jax import lax
from jax.experimental import pallas as pl
from jax.experimental.pallas import tpu as pltpu
from jax.sharding import PartitionSpec as P

ROWS = 16
COLS = 64
WIN = 20
EDGE = 8
MESH = pl.DeviceIdType.MESH
SLOT_A = 4
SLOT_S = 10
SLOT_X = 12
SLOT_H = 8
LATER = 6
EARLY = 11
HALO = 32


def shift_down(v, edge):
    rolled = pltpu.roll(v, 1, axis=0)
    pos = lax.broadcasted_iota(jnp.int32, v.shape, 0) % COLS
    return jnp.where(pos == 0, edge, rolled)


def shift_up(v, edge):
    rolled = pltpu.roll(v, v.shape[0] - 1, axis=0)
    pos = lax.broadcasted_iota(jnp.int32, v.shape, 0) % COLS
    return jnp.where(pos == COLS - 1, edge, rolled)


def build_half(is_left, xc, hx, x3, xh):
    for r in range(WIN):
        mid = xc[2 + r]
        v = mid.astype(jnp.float32)
        h = hx[r].astype(jnp.float32)
        near = jnp.where(is_left, h[0:1], h[EDGE - 1:EDGE])
        far = jnp.where(is_left, h[1:2], h[EDGE - 2:EDGE - 1])
        own = jnp.where(is_left, v[COLS - 1:COLS], v[0:1])
        zero = jnp.zeros_like(near)
        rows = pl.ds(r * COLS, COLS)
        x3[rows, 0:128] = shift_down(v, jnp.where(is_left, zero, near)).astype(jnp.bfloat16)
        x3[rows, 128:256] = mid
        x3[rows, 256:384] = shift_up(v, jnp.where(is_left, near, zero)).astype(jnp.bfloat16)
        xh[r:r + 1, 0:128] = jnp.where(is_left, own, far)
        xh[r:r + 1, 128:256] = near
        xh[r:r + 1, 256:384] = jnp.where(is_left, far, own)


def build_x3(is_left, xc, hx, x3, xh):
    for half in range(2):
        build_half(is_left, xc.at[half], hx.at[half], x3.at[half], xh.at[half])


BLOCKS = ((0, 10), (10, 8))


def lhs_rows(x3s, xhs, first, count):
    m = count * COLS
    lhs = jnp.concatenate([x3[(first + dy) * COLS:(first + dy) * COLS + m, :] for x3 in x3s for dy in range(3)], axis=1)
    if first == 0:
        edge = jnp.concatenate([xh[dy:dy + HALO, :] for xh in xhs for dy in range(3)], axis=1).astype(jnp.bfloat16)
        lhs = jnp.concatenate([edge, lhs], axis=0)
    return lhs


def part_rows(first, count):
    start = 0 if first == 0 else HALO + first * COLS
    return slice(start, HALO + (first + count) * COLS)


def conv1_part(x3, xh, w, zp):
    for first, count in BLOCKS:
        z = jnp.dot(lhs_rows([x3], [xh], first, count), w[...].reshape(1152, 512), preferred_element_type=jnp.float32)
        zp[part_rows(first, count), :] = z.astype(jnp.bfloat16)


def conv1(is_left, top, bottom, x3s, xhs, w, depth, b1, y3, zp=None):
    edge_all = None
    for first, count in BLOCKS:
        z = jnp.dot(lhs_rows(x3s, xhs, first, count), w[...].reshape(depth, 512), preferred_element_type=jnp.float32)
        if zp is not None:
            z = z + zp[part_rows(first, count), :].astype(jnp.float32)
        z = jnp.maximum(z + b1[...], 0.0)
        if first == 0:
            edge_all = z[:HALO]
            z = z[HALO:]
        for r in range(count):
            row = first + r
            v = z[r * COLS:(r + 1) * COLS]
            e = edge_all[row:row + 1]
            if row == 0:
                v = jnp.where(top, 0.0, v)
                e = jnp.where(top, 0.0, e)
            if row == ROWS + 1:
                v = jnp.where(bottom, 0.0, v)
                e = jnp.where(bottom, 0.0, e)
            zero = jnp.zeros_like(e)
            dst = pl.ds(row * COLS, COLS)
            y3[dst, 0:512] = shift_down(v, jnp.where(is_left, zero, e)).astype(jnp.bfloat16)
            y3[dst, 512:1024] = v.astype(jnp.bfloat16)
            y3[dst, 1024:1536] = shift_up(v, jnp.where(is_left, e, zero)).astype(jnp.bfloat16)


def conv2(y3, w2, b2, out, blk=8):
    for first in range(0, ROWS, blk):
        m = blk * COLS
        lhs = jnp.concatenate([y3[(first + dy) * COLS:(first + dy) * COLS + m, :] for dy in range(3)], axis=1)
        out[first * COLS:first * COLS + m, :] = jnp.dot(lhs, w2[...], preferred_element_type=jnp.float32) + b2[...]


def merge(slot, chip, off, ab, xc_slot, sb_slot):
    for r in range(WIN):
        xc_slot[chip, off + r] = jnp.concatenate([ab[slot, 0, 0, r], ab[slot, 0, 1, r]], axis=-1)
        sb_slot[r] = jnp.concatenate([ab[slot, 1, 0, r], ab[slot, 1, 1, r]], axis=-1)


def fused_kernel(images, x, w1, b1, w2, b2, y, x_rest, h_rest, w1_all, ab, sb, xc, hx, x3, xh, y3, ob, w1v, w2v, hp, zp,
                 loc_sem, a_send, a_recv, x_send, x_recv, h_send, h_recv, o_sem, w_loc, w_send, w_recv, rest_sem, p_send, p_recv,
                 credit_a, credit_x, credit_h):
    now = images - LATER
    data = lax.axis_index('data')
    side = lax.axis_index('cols')
    model = lax.axis_index('model')
    is_left = side == 0
    chip = model // 2
    core = model % 2
    mate = chip * 2 + 1 - core
    far = (1 - chip) * 2 + core
    far_mate = (1 - chip) * 2 + 1 - core
    to_mate = (data, side, mate)
    to_far = (data, side, far)
    to_side = (data, 1 - side, model)

    def source(m):
        return jnp.where(m == 0, 0, jnp.where(m == 3, 44, ROWS * m - 2))

    def place(m):
        return jnp.where(m == 0, 4, jnp.where(m == 3, 0, 2))

    edge = pl.multiple_of(jnp.where(is_left, COLS - EDGE, 0), EDGE)

    for slot in range(SLOT_X):
        for half in range(2):
            for row in (2, 3, 20, 21):
                xc[slot, half, row] = jnp.zeros((COLS, 128), jnp.bfloat16)
    xh[...] = jnp.zeros_like(xh)

    barrier = pltpu.get_barrier_semaphore()
    for peer in (to_mate, to_far, to_side):
        pl.semaphore_signal(barrier, inc=1, device_id=peer, device_id_type=MESH)
    pl.semaphore_wait(barrier, 3)

    def remote(src, dst, send, recv, peer):
        return pltpu.make_async_remote_copy(src_ref=src, dst_ref=dst, send_sem=send, recv_sem=recv, device_id=peer, device_id_type=MESH)

    def w1_part(m):
        return w1v.at[m // 2, :, pl.ds(pl.multiple_of(m % 2 * 64, 64), 64), :]

    def w1_half(m, half):
        return w1v.at[m // 2, :, pl.ds(pl.multiple_of(m % 2 * 64, 64), 64), pl.ds(pl.multiple_of(half * 256, 256), 256)]

    w_far = remote(w1.at[:, :, pl.ds(pl.multiple_of(side * 256, 256), 256)], w1_half(model, side), w_send.at[0], w_recv.at[0], to_far)
    def w1_piece(half, piece):
        return w1_half(far, half).at[pl.ds(3 * piece, 3)]

    w_side = [remote(w1_piece(side, p), w1_piece(side, p), w_send.at[3 + p], w_recv.at[3 + p], to_side) for p in range(3)]
    w_pass = remote(w1_half(far, side), w1_half(far, side), w_send.at[2], w_recv.at[2], to_mate)
    w_last = [remote(w1_piece(1 - side, p), w1_piece(1 - side, p), w_send.at[6 + p], w_recv.at[6 + p], to_mate) for p in range(3)]
    w_mate = remote(w1, w1_part(model), w_send.at[1], w_recv.at[1], to_mate)
    w_own = pltpu.make_async_copy(w1, w1_part(model), w_loc.at[0])
    w2_own = pltpu.make_async_copy(w2, w2v, w_loc.at[1])

    def own_copy(n, win):
        slot = n % SLOT_A
        rows = pl.ds(source(model if win == 0 else far), WIN)
        return pltpu.make_async_copy(x.at[n, rows], ab.at[slot, win, core], loc_sem.at[slot, win])

    def mate_copy(n, win):
        slot = n % SLOT_A
        rows = pl.ds(source(mate if win == 0 else far_mate), WIN)
        return remote(x.at[n, rows], ab.at[slot, win, core], a_send.at[slot, win], a_recv.at[slot, win], to_mate)

    def is_edge(m):
        return jnp.logical_or(m == 0, m == 3)

    def by_size(m, run):
        @pl.when(is_edge(m))
        def _():
            run(WIN - 2, jnp.where(m == 3, 2, 0))

        @pl.when(jnp.logical_not(is_edge(m)))
        def _():
            run(WIN, 0)

    def far_copy(n, m, half, count, first):
        slot = n % SLOT_X
        return remote(sb.at[n % SLOT_S, pl.ds(first, count)], xc.at[slot, half, pl.ds(place(m) + first, count)],
                      x_send.at[slot], x_recv.at[slot], to_far)

    def side_copy(n):
        slot = n % SLOT_H
        return remote(xc.at[n % SLOT_X, :, pl.ds(2, WIN), pl.ds(edge, EDGE), :], hx.at[slot], h_send.at[slot], h_recv.at[slot], to_side)

    def out_copy(n):
        return pltpu.make_async_copy(ob.at[n % 2], y.at[n], o_sem.at[n % 2])

    def rest_copy(n, part):
        if part == 0:
            return pltpu.make_async_copy(xc.at[n % SLOT_X, :, pl.ds(2, WIN)], x_rest.at[n - now], rest_sem.at[n - now, 0])
        return pltpu.make_async_copy(hx.at[n % SLOT_H], h_rest.at[n - now], rest_sem.at[n - now, 1])

    def seen(i):
        return i + 2 + jnp.maximum(i - 12, 0) // 6

    def each(i, run):
        lo, hi = seen(i - 1), seen(i)
        run(lo + 1)

        @pl.when(hi > lo + 1)
        def _():
            run(lo + 2)

    def start_a(n):
        @pl.when(n >= SLOT_A)
        def _():
            pl.semaphore_wait(credit_a, 1)
        for win in range(2):
            own_copy(n, win).start()
            mate_copy(n, win).start()

    def start_x(n):
        @pl.when(n >= SLOT_X)
        def _():
            pl.semaphore_wait(credit_x, 1)
        by_size(far, lambda count, first: far_copy(n, far, chip, count, first).start())

    def wait_a(n):
        for win in range(2):
            own_copy(n, win).wait()
            mate_copy(n, win).wait()

    def start_h(n):
        by_size(far, lambda count, first: far_copy(n, far, chip, count, first).wait_send())
        by_size(model, lambda count, first: far_copy(n, model, 1 - chip, count, first).wait_recv())

        @pl.when(n >= SLOT_H)
        def _():
            pl.semaphore_wait(credit_h, 1)
        side_copy(n).start()

    def wait_h(n):
        side_copy(n).wait()

        @pl.when(n >= now)
        def _():
            rest_copy(n, 0).start()
            rest_copy(n, 1).start()

    def part_copy(n):
        return remote(xc.at[n % SLOT_X, chip, pl.ds(2, WIN), pl.ds(edge, EDGE), :], hp.at[n], p_send.at[n], p_recv.at[n], to_side)

    def control(i):
        @pl.when(i + EARLY + 1 < images)
        def _():
            start_a(i + EARLY + 1)

        @pl.when(jnp.logical_and(i >= 1, i + EARLY - 1 < images))
        def _():
            start_x(i + EARLY - 1)

        @pl.when(i + EARLY < images)
        def _():
            wait_a(i + EARLY)
        each(i, start_h)
        each(i - 1, wait_h)

    def free_a(n):
        @pl.when(n < images - SLOT_A)
        def _():
            pl.semaphore_signal(credit_a, inc=1, device_id=to_mate, device_id_type=MESH)

    def free_built(n):
        @pl.when(n < images - SLOT_X)
        def _():
            pl.semaphore_signal(credit_x, inc=1, device_id=to_far, device_id_type=MESH)

        @pl.when(n < images - SLOT_H)
        def _():
            pl.semaphore_signal(credit_h, inc=1, device_id=to_side, device_id_type=MESH)

    def do_merge(n, live):
        merge(n % SLOT_A, chip, place(model), ab, xc.at[jnp.where(live, n % SLOT_X, SLOT_X)], sb.at[jnp.where(live, n % SLOT_S, SLOT_S)])

    def do_build(n):
        build_x3(is_left, xc.at[n % SLOT_X], hx.at[n % SLOT_H], x3, xh)

    w_far.start()
    w_mate.start()
    w_own.start()
    w2_own.start()

    for n in range(3):
        start_a(n)
    w_own.wait()
    w_mate.wait()

    def fill(t, _):
        @pl.when(t < EARLY)
        def _():
            wait_a(t)

        @pl.when(jnp.logical_and(t >= 1, t <= EARLY))
        def _():
            start_x(t - 1)
            part_copy(t - 1).start()

        @pl.when(t + 3 <= EARLY)
        def _():
            start_a(t + 3)

        @pl.when(t == 5)
        def _():
            w_far.wait()
            w_pass.start()
        for p in range(3):
            @pl.when(t == 5 + p)
            def _():
                w_side[p].start()

            @pl.when(t == 7 + p)
            def _():
                w_side[p].wait()
                w_last[p].start()

        @pl.when(t == 9)
        def _():
            start_h(0)

        @pl.when(t == EARLY + 2)
        def _():
            start_h(1)

        @pl.when(jnp.logical_and(t >= 2, t < EARLY + 2))
        def _():
            part_copy(t - 2).wait()

        def build_part(n):
            build_half(is_left, xc.at[n % SLOT_X, chip], hp.at[n], x3.at[chip], xh.at[chip])

        @pl.when(t < 3)
        def _():
            do_merge(t, True)

        @pl.when(t == 2)
        def _():
            build_part(0)

        @pl.when(t >= 3)
        def _():
            conv1_part(x3.at[chip], xh.at[chip], w1v.at[chip], zp.at[t - 3])
            build_part(jnp.minimum(t - 2, EARLY - 1))
            do_merge(jnp.minimum(t, EARLY - 1), t < EARLY)

        @pl.when(t < EARLY)
        def _():
            free_a(t)
        return 0

    lax.fori_loop(0, EARLY + 3, fill, 0)
    w2_own.wait()
    for copy in [w_pass] + w_last:
        copy.wait()
    wait_h(0)
    do_build(0)
    free_built(0)
    w_out = pltpu.make_async_copy(w1v, w1_all, w_loc.at[2])
    w_out.start()

    def step(early, i, _):
        control(i)

        @pl.when(i >= 2)
        def _():
            out_copy(i - 2).wait()
        if early:
            conv1(is_left, model == 0, model == 3, [x3.at[1 - chip]], [xh.at[1 - chip]], w1v.at[1 - chip], 1152, b1, y3, zp.at[i])
        else:
            conv1(is_left, model == 0, model == 3, [x3.at[0], x3.at[1]], [xh.at[0], xh.at[1]], w1v, 2304, b1, y3)
        do_build(i + 1)
        do_merge(i + EARLY, i + EARLY < images)
        conv2(y3, w2v, b2, ob.at[i % 2])
        out_copy(i).start()

        @pl.when(i + EARLY < images)
        def _():
            free_a(i + EARLY)
        free_built(i + 1)
        return 0

    lax.fori_loop(0, EARLY, functools.partial(step, True), 0)
    lax.fori_loop(EARLY, now, functools.partial(step, False), 0)
    for n in range(images - 2, images):
        start_h(n)
    each(now - 1, wait_h)
    for n in range(images - 2, images):
        wait_h(n)
    out_copy(now - 2).wait()
    out_copy(now - 1).wait()
    w_out.wait()
    for n in range(now, images):
        rest_copy(n, 0).wait()
        rest_copy(n, 1).wait()


def rest_kernel(images, y_done, x_rest, h_rest, w1, b1, w2, b2, y, xc, hx, x3, xh, y3, ob, w1v, w2v, cb,
                l_sem, w_sem, o_sem, in_sem, out_sem):
    done = images - LATER
    sets = LATER - 1
    size = -(-done // sets)
    model = lax.axis_index('model')
    is_left = lax.axis_index('cols') == 0
    weights = [pltpu.make_async_copy(w1, w1v, w_sem.at[0]), pltpu.make_async_copy(w2, w2v, w_sem.at[1])]
    xh[...] = jnp.zeros_like(xh)

    def load(n):
        return [pltpu.make_async_copy(x_rest.at[n], xc.at[n, :, pl.ds(2, WIN)], l_sem.at[n, 0]),
                pltpu.make_async_copy(h_rest.at[n], hx.at[n], l_sem.at[n, 1])]

    def bring(s, q):
        return pltpu.make_async_copy(y_done.at[s + sets * q], cb.at[s % 2, q], in_sem.at[s % 2, q])

    def put(s, q):
        return pltpu.make_async_copy(cb.at[s % 2, q], y.at[s + sets * q], out_sem.at[s % 2, q])

    def each(s, run):
        for q in range(size):
            @pl.when(jnp.logical_and(jnp.logical_and(s >= 0, s < sets), s + sets * q < done))
            def _():
                run(s, q)

    def out_copy(n):
        return pltpu.make_async_copy(ob.at[n % 2], y.at[done + n], o_sem.at[n % 2])

    for copy in load(0) + weights[:1] + load(1) + weights[1:] + [c for n in range(2, LATER) for c in load(n)]:
        copy.start()
    for copy in load(0):
        copy.wait()
    build_x3(is_left, xc.at[0], hx.at[0], x3, xh)
    for copy in weights + [c for n in range(1, LATER) for c in load(n)]:
        copy.wait()

    def step(i, _):
        each(i - 1, lambda s, q: bring(s, q).wait())
        each(i - 1, lambda s, q: put(s, q).start())
        each(i - 2, lambda s, q: put(s, q).wait())
        each(i, lambda s, q: bring(s, q).start())

        @pl.when(i >= 2)
        def _():
            out_copy(i - 2).wait()
        conv1(is_left, model == 0, model == 3, [x3.at[0], x3.at[1]], [xh.at[0], xh.at[1]], w1v, 2304, b1, y3)
        n = jnp.minimum(i + 1, LATER - 1)
        build_x3(is_left, xc.at[n], hx.at[n], x3, xh)
        conv2(y3, w2v, b2, ob.at[i % 2])
        out_copy(i).start()
        return 0

    lax.fori_loop(0, LATER, step, 0)
    each(jnp.int32(sets - 1), lambda s, q: put(s, q).wait())
    out_copy(LATER - 2).wait()
    out_copy(LATER - 1).wait()


def rest(images, y_done, x_rest, h_rest, w1, b1, w2, b2):
    hbm = pl.BlockSpec(memory_space=pl.ANY)
    vmem = pl.BlockSpec(memory_space=pltpu.VMEM)
    dma = pltpu.SemaphoreType.DMA
    bf16 = jnp.bfloat16
    size = -(-(images - LATER) // (LATER - 1))
    return pl.pallas_call(
        functools.partial(rest_kernel, images),
        out_shape=jax.ShapeDtypeStruct((images, ROWS * COLS, 512), jnp.float32),
        in_specs=[hbm, hbm, hbm, hbm, vmem, hbm, vmem],
        out_specs=hbm,
        scratch_shapes=[
            pltpu.VMEM((LATER, 2, WIN + 4, COLS, 128), bf16),
            pltpu.VMEM((LATER, 2, WIN, EDGE, 128), bf16),
            pltpu.VMEM((2, WIN * COLS, 384), bf16),
            pltpu.VMEM((2, 40, 384), jnp.float32),
            pltpu.VMEM(((ROWS + 2) * COLS, 1536), bf16),
            pltpu.VMEM((2, ROWS * COLS, 512), jnp.float32),
            pltpu.VMEM((2, 9, 128, 512), bf16),
            pltpu.VMEM((4608, 512), bf16),
            pltpu.VMEM((2, size, ROWS * COLS, 512), jnp.float32),
            dma((LATER, 2)), dma((2,)), dma((2,)), dma((2, size)), dma((2, size)),
        ],
        compiler_params=pltpu.CompilerParams(vmem_limit_bytes=62 * 1024 * 1024),
    )(y_done, x_rest, h_rest, w1, b1, w2, b2)


def fused(x, w1, b1, w2, b2):
    images = x.shape[0]
    hbm = pl.BlockSpec(memory_space=pl.ANY)
    vmem = pl.BlockSpec(memory_space=pltpu.VMEM)
    dma = pltpu.SemaphoreType.DMA
    bf16 = jnp.bfloat16
    return pl.pallas_call(
        functools.partial(fused_kernel, images),
        out_shape=[
            jax.ShapeDtypeStruct((images - LATER, ROWS * COLS, 512), jnp.float32),
            jax.ShapeDtypeStruct((LATER, 2, WIN, COLS, 128), bf16),
            jax.ShapeDtypeStruct((LATER, 2, WIN, EDGE, 128), bf16),
            jax.ShapeDtypeStruct((2, 9, 128, 512), bf16),
        ],
        in_specs=[hbm, hbm, vmem, hbm, vmem],
        out_specs=[hbm] * 4,
        scratch_shapes=[
            pltpu.VMEM((SLOT_A, 2, 2, WIN, COLS, 64), bf16),
            pltpu.VMEM((SLOT_S + 1, WIN, COLS, 128), bf16),
            pltpu.VMEM((SLOT_X + 1, 2, WIN + 4, COLS, 128), bf16),
            pltpu.VMEM((SLOT_H, 2, WIN, EDGE, 128), bf16),
            pltpu.VMEM((2, WIN * COLS, 384), bf16),
            pltpu.VMEM((2, 40, 384), jnp.float32),
            pltpu.VMEM(((ROWS + 2) * COLS, 1536), bf16),
            pltpu.VMEM((2, ROWS * COLS, 512), jnp.float32),
            pltpu.VMEM((2, 9, 128, 512), bf16),
            pltpu.VMEM((4608, 512), bf16),
            pltpu.VMEM((EARLY, WIN, EDGE, 128), bf16),
            pltpu.VMEM((EARLY, HALO + (ROWS + 2) * COLS, 512), bf16),
            dma((SLOT_A, 2)), dma((SLOT_A, 2)), dma((SLOT_A, 2)),
            dma((SLOT_X,)), dma((SLOT_X,)), dma((SLOT_H,)), dma((SLOT_H,)), dma((2,)),
            dma((3,)), dma((9,)), dma((9,)), dma((LATER, 2)), dma((EARLY,)), dma((EARLY,)),
            pltpu.SemaphoreType.REGULAR, pltpu.SemaphoreType.REGULAR, pltpu.SemaphoreType.REGULAR,
        ],
        compiler_params=pltpu.CompilerParams(vmem_limit_bytes=60 * 1024 * 1024, collective_id=0, has_side_effects=True),
    )(x, w1, b1, w2, b2)


def solution(mesh):
    def local_step(x, w1, b1, w2, b2):
        images = x.shape[0]
        b1, w2, b2 = b1.reshape(1, 512), w2.reshape(4608, 512), b2.reshape(1, 512)
        done, x_rest, h_rest, w1_all = fused(x, w1.reshape(9, 64, 512), b1, w2, b2)
        y = rest(images, done, x_rest, h_rest, w1_all, b1, w2, b2)
        return y.reshape(images, ROWS, COLS, 512)

    return jax.shard_map(local_step, mesh=mesh, in_specs=(P('data', None, 'cols', 'model'), P(None, None, 'model', None), P(), P(), P()), out_specs=P('data', 'model', 'cols', None), check_vma=False)
```

```python
import functools

import jax
import jax.numpy as jnp
from jax import lax
from jax.experimental import pallas as pl
from jax.experimental.pallas import tpu as pltpu
from jax.sharding import PartitionSpec as P

ROWS = 16
COLS = 64
WIN = 20
EDGE = 8
MESH = pl.DeviceIdType.MESH
SLOT_A = 4
SLOT_S = 10
SLOT_X = 12
SLOT_H = 8
LATER = 6
EARLY = 6
HALO = 32


def shift_down(v, edge):
    rolled = pltpu.roll(v, 1, axis=0)
    pos = lax.broadcasted_iota(jnp.int32, v.shape, 0) % COLS
    return jnp.where(pos == 0, edge, rolled)


def shift_up(v, edge):
    rolled = pltpu.roll(v, v.shape[0] - 1, axis=0)
    pos = lax.broadcasted_iota(jnp.int32, v.shape, 0) % COLS
    return jnp.where(pos == COLS - 1, edge, rolled)


def build_half(is_left, xc, hx, x3, xh):
    for r in range(WIN):
        mid = xc[2 + r]
        v = mid.astype(jnp.float32)
        h = hx[r].astype(jnp.float32)
        near = jnp.where(is_left, h[0:1], h[EDGE - 1:EDGE])
        far = jnp.where(is_left, h[1:2], h[EDGE - 2:EDGE - 1])
        own = jnp.where(is_left, v[COLS - 1:COLS], v[0:1])
        zero = jnp.zeros_like(near)
        rows = pl.ds(r * COLS, COLS)
        x3[rows, 0:128] = shift_down(v, jnp.where(is_left, zero, near)).astype(jnp.bfloat16)
        x3[rows, 128:256] = mid
        x3[rows, 256:384] = shift_up(v, jnp.where(is_left, near, zero)).astype(jnp.bfloat16)
        xh[r:r + 1, 0:128] = jnp.where(is_left, own, far)
        xh[r:r + 1, 128:256] = near
        xh[r:r + 1, 256:384] = jnp.where(is_left, far, own)


def build_x3(is_left, xc, hx, x3, xh):
    for half in range(2):
        build_half(is_left, xc.at[half], hx.at[half], x3.at[half], xh.at[half])


BLOCKS = ((0, 10), (10, 8))


def lhs_rows(x3s, xhs, first, count):
    m = count * COLS
    lhs = jnp.concatenate([x3[(first + dy) * COLS:(first + dy) * COLS + m, :] for x3 in x3s for dy in range(3)], axis=1)
    if first == 0:
        edge = jnp.concatenate([xh[dy:dy + HALO, :] for xh in xhs for dy in range(3)], axis=1).astype(jnp.bfloat16)
        lhs = jnp.concatenate([edge, lhs], axis=0)
    return lhs


def part_rows(first, count):
    start = 0 if first == 0 else HALO + first * COLS
    return slice(start, HALO + (first + count) * COLS)


def conv1_part(x3, xh, w, zp):
    for first, count in BLOCKS:
        z = jnp.dot(lhs_rows([x3], [xh], first, count), w[...].reshape(1152, 512), preferred_element_type=jnp.float32)
        zp[part_rows(first, count), :] = z.astype(jnp.bfloat16)


def conv1(is_left, top, bottom, x3s, xhs, w, depth, b1, y3, zp=None):
    edge_all = None
    for first, count in BLOCKS:
        z = jnp.dot(lhs_rows(x3s, xhs, first, count), w[...].reshape(depth, 512), preferred_element_type=jnp.float32)
        if zp is not None:
            z = z + zp[part_rows(first, count), :].astype(jnp.float32)
        z = jnp.maximum(z + b1[...], 0.0)
        if first == 0:
            edge_all = z[:HALO]
            z = z[HALO:]
        for r in range(count):
            row = first + r
            v = z[r * COLS:(r + 1) * COLS]
            e = edge_all[row:row + 1]
            if row == 0:
                v = jnp.where(top, 0.0, v)
                e = jnp.where(top, 0.0, e)
            if row == ROWS + 1:
                v = jnp.where(bottom, 0.0, v)
                e = jnp.where(bottom, 0.0, e)
            zero = jnp.zeros_like(e)
            dst = pl.ds(row * COLS, COLS)
            y3[dst, 0:512] = shift_down(v, jnp.where(is_left, zero, e)).astype(jnp.bfloat16)
            y3[dst, 512:1024] = v.astype(jnp.bfloat16)
            y3[dst, 1024:1536] = shift_up(v, jnp.where(is_left, e, zero)).astype(jnp.bfloat16)


def conv2(y3, w2, b2, out, blk=8):
    for first in range(0, ROWS, blk):
        m = blk * COLS
        lhs = jnp.concatenate([y3[(first + dy) * COLS:(first + dy) * COLS + m, :] for dy in range(3)], axis=1)
        out[first * COLS:first * COLS + m, :] = jnp.dot(lhs, w2[...], preferred_element_type=jnp.float32) + b2[...]


def merge(slot, chip, off, ab, xc_slot, sb_slot):
    for r in range(WIN):
        xc_slot[chip, off + r] = jnp.concatenate([ab[slot, 0, 0, r], ab[slot, 0, 1, r]], axis=-1)
        sb_slot[r] = jnp.concatenate([ab[slot, 1, 0, r], ab[slot, 1, 1, r]], axis=-1)


def fused_kernel(images, x, w1, b1, w2, b2, y, x_rest, h_rest, w1_all, ab, sb, xc, hx, x3, xh, y3, ob, w1v, w2v, hp, zp,
                 loc_sem, a_send, a_recv, x_send, x_recv, h_send, h_recv, o_sem, w_loc, w_send, w_recv, rest_sem, p_send, p_recv,
                 credit_a, credit_x, credit_h):
    now = images - LATER
    data = lax.axis_index('data')
    side = lax.axis_index('cols')
    model = lax.axis_index('model')
    is_left = side == 0
    chip = model // 2
    core = model % 2
    mate = chip * 2 + 1 - core
    far = (1 - chip) * 2 + core
    far_mate = (1 - chip) * 2 + 1 - core
    to_mate = (data, side, mate)
    to_far = (data, side, far)
    to_side = (data, 1 - side, model)

    def source(m):
        return jnp.where(m == 0, 0, jnp.where(m == 3, 44, ROWS * m - 2))

    def place(m):
        return jnp.where(m == 0, 4, jnp.where(m == 3, 0, 2))

    edge = pl.multiple_of(jnp.where(is_left, COLS - EDGE, 0), EDGE)

    for slot in range(SLOT_X):
        for half in range(2):
            for row in (2, 3, 20, 21):
                xc[slot, half, row] = jnp.zeros((COLS, 128), jnp.bfloat16)
    xh[...] = jnp.zeros_like(xh)

    barrier = pltpu.get_barrier_semaphore()
    for peer in (to_mate, to_far, to_side):
        pl.semaphore_signal(barrier, inc=1, device_id=peer, device_id_type=MESH)
    pl.semaphore_wait(barrier, 3)

    def remote(src, dst, send, recv, peer):
        return pltpu.make_async_remote_copy(src_ref=src, dst_ref=dst, send_sem=send, recv_sem=recv, device_id=peer, device_id_type=MESH)

    def w1_part(m):
        return w1v.at[m // 2, :, pl.ds(pl.multiple_of(m % 2 * 64, 64), 64), :]

    def w1_half(m, half):
        return w1v.at[m // 2, :, pl.ds(pl.multiple_of(m % 2 * 64, 64), 64), pl.ds(pl.multiple_of(half * 256, 256), 256)]

    w_far = remote(w1.at[:, :, pl.ds(pl.multiple_of(side * 256, 256), 256)], w1_half(model, side), w_send.at[0], w_recv.at[0], to_far)
    def w1_piece(half, piece):
        return w1_half(far, half).at[pl.ds(3 * piece, 3)]

    w_side = [remote(w1_piece(side, p), w1_piece(side, p), w_send.at[3 + p], w_recv.at[3 + p], to_side) for p in range(3)]
    w_pass = remote(w1_half(far, side), w1_half(far, side), w_send.at[2], w_recv.at[2], to_mate)
    w_last = [remote(w1_piece(1 - side, p), w1_piece(1 - side, p), w_send.at[6 + p], w_recv.at[6 + p], to_mate) for p in range(3)]
    w_mate = remote(w1, w1_part(model), w_send.at[1], w_recv.at[1], to_mate)
    w_own = pltpu.make_async_copy(w1, w1_part(model), w_loc.at[0])
    w2_own = pltpu.make_async_copy(w2, w2v, w_loc.at[1])

    def own_copy(n, win):
        slot = n % SLOT_A
        rows = pl.ds(source(model if win == 0 else far), WIN)
        return pltpu.make_async_copy(x.at[n, rows], ab.at[slot, win, core], loc_sem.at[slot, win])

    def mate_copy(n, win):
        slot = n % SLOT_A
        rows = pl.ds(source(mate if win == 0 else far_mate), WIN)
        return remote(x.at[n, rows], ab.at[slot, win, core], a_send.at[slot, win], a_recv.at[slot, win], to_mate)

    def is_edge(m):
        return jnp.logical_or(m == 0, m == 3)

    def by_size(m, run):
        @pl.when(is_edge(m))
        def _():
            run(WIN - 2, jnp.where(m == 3, 2, 0))

        @pl.when(jnp.logical_not(is_edge(m)))
        def _():
            run(WIN, 0)

    def far_copy(n, m, half, count, first):
        slot = n % SLOT_X
        return remote(sb.at[n % SLOT_S, pl.ds(first, count)], xc.at[slot, half, pl.ds(place(m) + first, count)],
                      x_send.at[slot], x_recv.at[slot], to_far)

    def side_copy(n):
        slot = n % SLOT_H
        return remote(xc.at[n % SLOT_X, :, pl.ds(2, WIN), pl.ds(edge, EDGE), :], hx.at[slot], h_send.at[slot], h_recv.at[slot], to_side)

    def out_copy(n):
        return pltpu.make_async_copy(ob.at[n % 2], y.at[n], o_sem.at[n % 2])

    def rest_copy(n, part):
        if part == 0:
            return pltpu.make_async_copy(xc.at[n % SLOT_X, :, pl.ds(2, WIN)], x_rest.at[n - now], rest_sem.at[n - now, 0])
        return pltpu.make_async_copy(hx.at[n % SLOT_H], h_rest.at[n - now], rest_sem.at[n - now, 1])

    def seen(i):
        return i + 2 + jnp.maximum(i - 10, 0) // 5

    def each(i, run):
        lo, hi = seen(i - 1), seen(i)
        run(lo + 1)

        @pl.when(hi > lo + 1)
        def _():
            run(lo + 2)

    def last(i):
        return jnp.minimum(i + EARLY + 1 + jnp.maximum(i, 0) // 4, images - 1)

    def batch(i, run):
        lo, hi = last(i - 1), last(i)

        @pl.when(hi > lo)
        def _():
            run(lo + 1)

        @pl.when(hi > lo + 1)
        def _():
            run(lo + 2)

    def start_a(n):
        @pl.when(n >= SLOT_A)
        def _():
            pl.semaphore_wait(credit_a, 1)
        for win in range(2):
            own_copy(n, win).start()
            mate_copy(n, win).start()

    def start_x(n):
        @pl.when(n >= SLOT_X)
        def _():
            pl.semaphore_wait(credit_x, 1)
        by_size(far, lambda count, first: far_copy(n, far, chip, count, first).start())

    def wait_a(n):
        for win in range(2):
            own_copy(n, win).wait()
            mate_copy(n, win).wait()

    def start_h(n):
        by_size(far, lambda count, first: far_copy(n, far, chip, count, first).wait_send())
        by_size(model, lambda count, first: far_copy(n, model, 1 - chip, count, first).wait_recv())

        @pl.when(n >= SLOT_H)
        def _():
            pl.semaphore_wait(credit_h, 1)
        side_copy(n).start()

    def wait_h(n):
        side_copy(n).wait()

        @pl.when(n >= now)
        def _():
            rest_copy(n, 0).start()
            rest_copy(n, 1).start()

    def part_copy(n):
        return remote(xc.at[n % SLOT_X, chip, pl.ds(2, WIN), pl.ds(edge, EDGE), :], hp.at[n], p_send.at[n], p_recv.at[n], to_side)

    def control(i):
        batch(i, start_a)

        @pl.when(i >= 1)
        def _():
            batch(i - 2, start_x)
        batch(i - 1, wait_a)

        @pl.when(last(i - 1) > last(i - 2) + 1)
        def _():
            do_merge(last(i - 1) - 1, True)
        each(i, start_h)
        each(i - 1, wait_h)

    def free_a(n):
        @pl.when(n < images - SLOT_A)
        def _():
            pl.semaphore_signal(credit_a, inc=1, device_id=to_mate, device_id_type=MESH)

    def free_built(n):
        @pl.when(n < images - SLOT_X)
        def _():
            pl.semaphore_signal(credit_x, inc=1, device_id=to_far, device_id_type=MESH)

        @pl.when(n < images - SLOT_H)
        def _():
            pl.semaphore_signal(credit_h, inc=1, device_id=to_side, device_id_type=MESH)

    def do_merge(n, live):
        merge(n % SLOT_A, chip, place(model), ab, xc.at[jnp.where(live, n % SLOT_X, SLOT_X)], sb.at[jnp.where(live, n % SLOT_S, SLOT_S)])

    def do_build(n):
        build_x3(is_left, xc.at[n % SLOT_X], hx.at[n % SLOT_H], x3, xh)

    w_far.start()
    w_mate.start()
    w_own.start()
    w2_own.start()

    for n in range(3):
        start_a(n)
    w_own.wait()
    w_mate.wait()

    def fill(t, _):
        @pl.when(t < EARLY)
        def _():
            wait_a(t)

        @pl.when(jnp.logical_and(t >= 1, t <= EARLY))
        def _():
            start_x(t - 1)
            part_copy(t - 1).start()

        @pl.when(t + 3 <= EARLY)
        def _():
            start_a(t + 3)

        @pl.when(t == 3)
        def _():
            w_far.wait()
            w_pass.start()

        @pl.when(t == EARLY + 2)
        def _():
            for p in range(3):
                w_side[p].wait()
                w_last[p].start()
        for p in range(3):
            @pl.when(t == 3 + p)
            def _():
                w_side[p].start()

        @pl.when(t == EARLY + 1)
        def _():
            start_h(0)

        @pl.when(t == EARLY + 2)
        def _():
            start_h(1)

        @pl.when(jnp.logical_and(t >= 2, t < EARLY + 2))
        def _():
            part_copy(t - 2).wait()

        def build_part(n):
            build_half(is_left, xc.at[n % SLOT_X, chip], hp.at[n], x3.at[chip], xh.at[chip])

        @pl.when(t < 3)
        def _():
            do_merge(t, True)

        @pl.when(t == 2)
        def _():
            build_part(0)

        @pl.when(t >= 3)
        def _():
            conv1_part(x3.at[chip], xh.at[chip], w1v.at[chip], zp.at[t - 3])
            build_part(jnp.minimum(t - 2, EARLY - 1))
            do_merge(jnp.minimum(t, EARLY - 1), t < EARLY)

        @pl.when(t < EARLY)
        def _():
            free_a(t)
        return 0

    lax.fori_loop(0, EARLY + 3, fill, 0)
    w2_own.wait()
    for copy in [w_pass] + w_last:
        copy.wait()
    wait_h(0)
    do_build(0)
    free_built(0)
    w_out = pltpu.make_async_copy(w1v, w1_all, w_loc.at[2])
    w_out.start()

    def step(early, i, _):
        control(i)

        @pl.when(i >= 2)
        def _():
            out_copy(i - 2).wait()
        if early:
            conv1(is_left, model == 0, model == 3, [x3.at[1 - chip]], [xh.at[1 - chip]], w1v.at[1 - chip], 1152, b1, y3, zp.at[i])
        else:
            conv1(is_left, model == 0, model == 3, [x3.at[0], x3.at[1]], [xh.at[0], xh.at[1]], w1v, 2304, b1, y3)
        do_build(i + 1)
        do_merge(last(i - 1), last(i - 1) > last(i - 2))
        conv2(y3, w2v, b2, ob.at[i % 2])
        out_copy(i).start()

        batch(i - 1, free_a)
        free_built(i + 1)
        return 0

    lax.fori_loop(0, EARLY, functools.partial(step, True), 0)
    lax.fori_loop(EARLY, now, functools.partial(step, False), 0)
    late = images - 1
    start_h(late)
    each(now - 1, wait_h)
    wait_h(late)
    out_copy(now - 2).wait()
    out_copy(now - 1).wait()
    w_out.wait()
    for n in range(now, images):
        rest_copy(n, 0).wait()
        rest_copy(n, 1).wait()


def rest_kernel(images, y_done, x_rest, h_rest, w1, b1, w2, b2, y, xc, hx, x3, xh, y3, ob, w1v, w2v, cb,
                l_sem, w_sem, o_sem, in_sem, out_sem):
    done = images - LATER
    sets = LATER - 1
    size = -(-done // sets)
    model = lax.axis_index('model')
    is_left = lax.axis_index('cols') == 0
    weights = [pltpu.make_async_copy(w1, w1v, w_sem.at[0]), pltpu.make_async_copy(w2, w2v, w_sem.at[1])]
    xh[...] = jnp.zeros_like(xh)

    def load(n):
        return [pltpu.make_async_copy(x_rest.at[n], xc.at[n, :, pl.ds(2, WIN)], l_sem.at[n, 0]),
                pltpu.make_async_copy(h_rest.at[n], hx.at[n], l_sem.at[n, 1])]

    def bring(s, q):
        return pltpu.make_async_copy(y_done.at[s + sets * q], cb.at[s % 2, q], in_sem.at[s % 2, q])

    def put(s, q):
        return pltpu.make_async_copy(cb.at[s % 2, q], y.at[s + sets * q], out_sem.at[s % 2, q])

    def each(s, run):
        for q in range(size):
            @pl.when(jnp.logical_and(jnp.logical_and(s >= 0, s < sets), s + sets * q < done))
            def _():
                run(s, q)

    def out_copy(n):
        return pltpu.make_async_copy(ob.at[n % 2], y.at[done + n], o_sem.at[n % 2])

    for copy in load(0) + weights[:1] + load(1) + weights[1:] + [c for n in range(2, LATER) for c in load(n)]:
        copy.start()
    for copy in load(0):
        copy.wait()
    build_x3(is_left, xc.at[0], hx.at[0], x3, xh)
    for copy in weights + [c for n in range(1, LATER) for c in load(n)]:
        copy.wait()

    def step(i, _):
        each(i - 1, lambda s, q: bring(s, q).wait())
        each(i - 1, lambda s, q: put(s, q).start())
        each(i - 2, lambda s, q: put(s, q).wait())
        each(i, lambda s, q: bring(s, q).start())

        @pl.when(i >= 2)
        def _():
            out_copy(i - 2).wait()
        conv1(is_left, model == 0, model == 3, [x3.at[0], x3.at[1]], [xh.at[0], xh.at[1]], w1v, 2304, b1, y3)
        n = jnp.minimum(i + 1, LATER - 1)
        build_x3(is_left, xc.at[n], hx.at[n], x3, xh)
        conv2(y3, w2v, b2, ob.at[i % 2])
        out_copy(i).start()
        return 0

    lax.fori_loop(0, LATER, step, 0)
    each(jnp.int32(sets - 1), lambda s, q: put(s, q).wait())
    out_copy(LATER - 2).wait()
    out_copy(LATER - 1).wait()


def rest(images, y_done, x_rest, h_rest, w1, b1, w2, b2):
    hbm = pl.BlockSpec(memory_space=pl.ANY)
    vmem = pl.BlockSpec(memory_space=pltpu.VMEM)
    dma = pltpu.SemaphoreType.DMA
    bf16 = jnp.bfloat16
    size = -(-(images - LATER) // (LATER - 1))
    return pl.pallas_call(
        functools.partial(rest_kernel, images),
        out_shape=jax.ShapeDtypeStruct((images, ROWS * COLS, 512), jnp.float32),
        in_specs=[hbm, hbm, hbm, hbm, vmem, hbm, vmem],
        out_specs=hbm,
        scratch_shapes=[
            pltpu.VMEM((LATER, 2, WIN + 4, COLS, 128), bf16),
            pltpu.VMEM((LATER, 2, WIN, EDGE, 128), bf16),
            pltpu.VMEM((2, WIN * COLS, 384), bf16),
            pltpu.VMEM((2, 40, 384), jnp.float32),
            pltpu.VMEM(((ROWS + 2) * COLS, 1536), bf16),
            pltpu.VMEM((2, ROWS * COLS, 512), jnp.float32),
            pltpu.VMEM((2, 9, 128, 512), bf16),
            pltpu.VMEM((4608, 512), bf16),
            pltpu.VMEM((2, size, ROWS * COLS, 512), jnp.float32),
            dma((LATER, 2)), dma((2,)), dma((2,)), dma((2, size)), dma((2, size)),
        ],
        compiler_params=pltpu.CompilerParams(vmem_limit_bytes=62 * 1024 * 1024),
    )(y_done, x_rest, h_rest, w1, b1, w2, b2)


def fused(x, w1, b1, w2, b2):
    images = x.shape[0]
    hbm = pl.BlockSpec(memory_space=pl.ANY)
    vmem = pl.BlockSpec(memory_space=pltpu.VMEM)
    dma = pltpu.SemaphoreType.DMA
    bf16 = jnp.bfloat16
    return pl.pallas_call(
        functools.partial(fused_kernel, images),
        out_shape=[
            jax.ShapeDtypeStruct((images - LATER, ROWS * COLS, 512), jnp.float32),
            jax.ShapeDtypeStruct((LATER, 2, WIN, COLS, 128), bf16),
            jax.ShapeDtypeStruct((LATER, 2, WIN, EDGE, 128), bf16),
            jax.ShapeDtypeStruct((2, 9, 128, 512), bf16),
        ],
        in_specs=[hbm, hbm, vmem, hbm, vmem],
        out_specs=[hbm] * 4,
        scratch_shapes=[
            pltpu.VMEM((SLOT_A, 2, 2, WIN, COLS, 64), bf16),
            pltpu.VMEM((SLOT_S + 1, WIN, COLS, 128), bf16),
            pltpu.VMEM((SLOT_X + 1, 2, WIN + 4, COLS, 128), bf16),
            pltpu.VMEM((SLOT_H, 2, WIN, EDGE, 128), bf16),
            pltpu.VMEM((2, WIN * COLS, 384), bf16),
            pltpu.VMEM((2, 40, 384), jnp.float32),
            pltpu.VMEM(((ROWS + 2) * COLS, 1536), bf16),
            pltpu.VMEM((2, ROWS * COLS, 512), jnp.float32),
            pltpu.VMEM((2, 9, 128, 512), bf16),
            pltpu.VMEM((4608, 512), bf16),
            pltpu.VMEM((EARLY, WIN, EDGE, 128), bf16),
            pltpu.VMEM((EARLY, HALO + (ROWS + 2) * COLS, 512), bf16),
            dma((SLOT_A, 2)), dma((SLOT_A, 2)), dma((SLOT_A, 2)),
            dma((SLOT_X,)), dma((SLOT_X,)), dma((SLOT_H,)), dma((SLOT_H,)), dma((2,)),
            dma((3,)), dma((9,)), dma((9,)), dma((LATER, 2)), dma((EARLY,)), dma((EARLY,)),
            pltpu.SemaphoreType.REGULAR, pltpu.SemaphoreType.REGULAR, pltpu.SemaphoreType.REGULAR,
        ],
        compiler_params=pltpu.CompilerParams(vmem_limit_bytes=60 * 1024 * 1024, collective_id=0, has_side_effects=True),
    )(x, w1, b1, w2, b2)


def solution(mesh):
    def local_step(x, w1, b1, w2, b2):
        images = x.shape[0]
        b1, w2, b2 = b1.reshape(1, 512), w2.reshape(4608, 512), b2.reshape(1, 512)
        done, x_rest, h_rest, w1_all = fused(x, w1.reshape(9, 64, 512), b1, w2, b2)
        y = rest(images, done, x_rest, h_rest, w1_all, b1, w2, b2)
        return y.reshape(images, ROWS, COLS, 512)

    return jax.shard_map(local_step, mesh=mesh, in_specs=(P('data', None, 'cols', 'model'), P(None, None, 'model', None), P(), P(), P()), out_specs=P('data', 'model', 'cols', None), check_vma=False)
```

```python
import functools

import jax
import jax.numpy as jnp
from jax import lax
from jax.experimental import pallas as pl
from jax.experimental.pallas import tpu as pltpu
from jax.sharding import PartitionSpec as P

ROWS = 16
COLS = 64
WIN = 20
EDGE = 8
MESH = pl.DeviceIdType.MESH
SLOT_A = 4
SLOT_S = 10
SLOT_X = 12
SLOT_H = 8
LATER = 6
EARLY = 5
HALO = 32


def shift_down(v, edge):
    rolled = pltpu.roll(v, 1, axis=0)
    pos = lax.broadcasted_iota(jnp.int32, v.shape, 0) % COLS
    return jnp.where(pos == 0, edge, rolled)


def shift_up(v, edge):
    rolled = pltpu.roll(v, v.shape[0] - 1, axis=0)
    pos = lax.broadcasted_iota(jnp.int32, v.shape, 0) % COLS
    return jnp.where(pos == COLS - 1, edge, rolled)


def build_half(is_left, xc, hx, x3, xh):
    for r in range(WIN):
        mid = xc[2 + r]
        v = mid.astype(jnp.float32)
        h = hx[r].astype(jnp.float32)
        near = jnp.where(is_left, h[0:1], h[EDGE - 1:EDGE])
        far = jnp.where(is_left, h[1:2], h[EDGE - 2:EDGE - 1])
        own = jnp.where(is_left, v[COLS - 1:COLS], v[0:1])
        zero = jnp.zeros_like(near)
        rows = pl.ds(r * COLS, COLS)
        x3[rows, 0:128] = shift_down(v, jnp.where(is_left, zero, near)).astype(jnp.bfloat16)
        x3[rows, 128:256] = mid
        x3[rows, 256:384] = shift_up(v, jnp.where(is_left, near, zero)).astype(jnp.bfloat16)
        xh[r:r + 1, 0:128] = jnp.where(is_left, own, far)
        xh[r:r + 1, 128:256] = near
        xh[r:r + 1, 256:384] = jnp.where(is_left, far, own)


def build_x3(is_left, xc, hx, x3, xh):
    for half in range(2):
        build_half(is_left, xc.at[half], hx.at[half], x3.at[half], xh.at[half])


BLOCKS = ((0, 10), (10, 8))


def lhs_rows(x3s, xhs, first, count):
    m = count * COLS
    lhs = jnp.concatenate([x3[(first + dy) * COLS:(first + dy) * COLS + m, :] for x3 in x3s for dy in range(3)], axis=1)
    if first == 0:
        edge = jnp.concatenate([xh[dy:dy + HALO, :] for xh in xhs for dy in range(3)], axis=1).astype(jnp.bfloat16)
        lhs = jnp.concatenate([edge, lhs], axis=0)
    return lhs


def part_rows(first, count):
    start = 0 if first == 0 else HALO + first * COLS
    return slice(start, HALO + (first + count) * COLS)


def conv1_part(x3, xh, w, zp):
    for first, count in BLOCKS:
        z = jnp.dot(lhs_rows([x3], [xh], first, count), w[...].reshape(1152, 512), preferred_element_type=jnp.float32)
        zp[part_rows(first, count), :] = z.astype(jnp.bfloat16)


def conv1(is_left, top, bottom, x3s, xhs, w, depth, b1, y3, zp=None):
    edge_all = None
    for first, count in BLOCKS:
        z = jnp.dot(lhs_rows(x3s, xhs, first, count), w[...].reshape(depth, 512), preferred_element_type=jnp.float32)
        if zp is not None:
            z = z + zp[part_rows(first, count), :].astype(jnp.float32)
        z = jnp.maximum(z + b1[...], 0.0)
        if first == 0:
            edge_all = z[:HALO]
            z = z[HALO:]
        for r in range(count):
            row = first + r
            v = z[r * COLS:(r + 1) * COLS]
            e = edge_all[row:row + 1]
            if row == 0:
                v = jnp.where(top, 0.0, v)
                e = jnp.where(top, 0.0, e)
            if row == ROWS + 1:
                v = jnp.where(bottom, 0.0, v)
                e = jnp.where(bottom, 0.0, e)
            zero = jnp.zeros_like(e)
            dst = pl.ds(row * COLS, COLS)
            y3[dst, 0:512] = shift_down(v, jnp.where(is_left, zero, e)).astype(jnp.bfloat16)
            y3[dst, 512:1024] = v.astype(jnp.bfloat16)
            y3[dst, 1024:1536] = shift_up(v, jnp.where(is_left, e, zero)).astype(jnp.bfloat16)


def conv2(y3, w2, b2, out, blk=8):
    for first in range(0, ROWS, blk):
        m = blk * COLS
        lhs = jnp.concatenate([y3[(first + dy) * COLS:(first + dy) * COLS + m, :] for dy in range(3)], axis=1)
        out[first * COLS:first * COLS + m, :] = jnp.dot(lhs, w2[...], preferred_element_type=jnp.float32) + b2[...]


def merge(slot, chip, off, ab, xc_slot, sb_slot):
    for r in range(WIN):
        xc_slot[chip, off + r] = jnp.concatenate([ab[slot, 0, 0, r], ab[slot, 0, 1, r]], axis=-1)
        sb_slot[r] = jnp.concatenate([ab[slot, 1, 0, r], ab[slot, 1, 1, r]], axis=-1)


def fused_kernel(images, x, w1, b1, w2, b2, y, x_rest, h_rest, w1_all, ab, sb, xc, hx, x3, xh, y3, ob, w1v, w2v, hp, zp,
                 loc_sem, a_send, a_recv, x_send, x_recv, h_send, h_recv, o_sem, w_loc, w_send, w_recv, rest_sem, p_send, p_recv,
                 credit_a, credit_x, credit_h):
    now = images - LATER
    data = lax.axis_index('data')
    side = lax.axis_index('cols')
    model = lax.axis_index('model')
    is_left = side == 0
    chip = model // 2
    core = model % 2
    mate = chip * 2 + 1 - core
    far = (1 - chip) * 2 + core
    far_mate = (1 - chip) * 2 + 1 - core
    to_mate = (data, side, mate)
    to_far = (data, side, far)
    to_side = (data, 1 - side, model)

    def source(m):
        return jnp.where(m == 0, 0, jnp.where(m == 3, 44, ROWS * m - 2))

    def place(m):
        return jnp.where(m == 0, 4, jnp.where(m == 3, 0, 2))

    edge = pl.multiple_of(jnp.where(is_left, COLS - EDGE, 0), EDGE)

    for slot in range(SLOT_X):
        for half in range(2):
            for row in (2, 3, 20, 21):
                xc[slot, half, row] = jnp.zeros((COLS, 128), jnp.bfloat16)
    xh[...] = jnp.zeros_like(xh)

    barrier = pltpu.get_barrier_semaphore()
    for peer in (to_mate, to_far, to_side):
        pl.semaphore_signal(barrier, inc=1, device_id=peer, device_id_type=MESH)
    pl.semaphore_wait(barrier, 3)

    def remote(src, dst, send, recv, peer):
        return pltpu.make_async_remote_copy(src_ref=src, dst_ref=dst, send_sem=send, recv_sem=recv, device_id=peer, device_id_type=MESH)

    def w1_part(m):
        return w1v.at[m // 2, :, pl.ds(pl.multiple_of(m % 2 * 64, 64), 64), :]

    def w1_half(m, half):
        return w1v.at[m // 2, :, pl.ds(pl.multiple_of(m % 2 * 64, 64), 64), pl.ds(pl.multiple_of(half * 256, 256), 256)]

    w_far = remote(w1.at[:, :, pl.ds(pl.multiple_of(side * 256, 256), 256)], w1_half(model, side), w_send.at[0], w_recv.at[0], to_far)
    def w1_piece(half, piece):
        return w1_half(far, half).at[pl.ds(3 * piece, 3)]

    w_side = [remote(w1_piece(side, p), w1_piece(side, p), w_send.at[3 + p], w_recv.at[3 + p], to_side) for p in range(3)]
    w_pass = remote(w1_half(far, side), w1_half(far, side), w_send.at[2], w_recv.at[2], to_mate)
    w_last = [remote(w1_piece(1 - side, p), w1_piece(1 - side, p), w_send.at[6 + p], w_recv.at[6 + p], to_mate) for p in range(3)]
    w_mate = remote(w1, w1_part(model), w_send.at[1], w_recv.at[1], to_mate)
    w_own = pltpu.make_async_copy(w1, w1_part(model), w_loc.at[0])
    w2_own = pltpu.make_async_copy(w2, w2v, w_loc.at[1])

    def own_copy(n, win):
        slot = n % SLOT_A
        rows = pl.ds(source(model if win == 0 else far), WIN)
        return pltpu.make_async_copy(x.at[n, rows], ab.at[slot, win, core], loc_sem.at[slot, win])

    def mate_copy(n, win):
        slot = n % SLOT_A
        rows = pl.ds(source(mate if win == 0 else far_mate), WIN)
        return remote(x.at[n, rows], ab.at[slot, win, core], a_send.at[slot, win], a_recv.at[slot, win], to_mate)

    def is_edge(m):
        return jnp.logical_or(m == 0, m == 3)

    def by_size(m, run):
        @pl.when(is_edge(m))
        def _():
            run(WIN - 2, jnp.where(m == 3, 2, 0))

        @pl.when(jnp.logical_not(is_edge(m)))
        def _():
            run(WIN, 0)

    def far_copy(n, m, half, count, first):
        slot = n % SLOT_X
        return remote(sb.at[n % SLOT_S, pl.ds(first, count)], xc.at[slot, half, pl.ds(place(m) + first, count)],
                      x_send.at[slot], x_recv.at[slot], to_far)

    def side_copy(n):
        slot = n % SLOT_H
        return remote(xc.at[n % SLOT_X, :, pl.ds(2, WIN), pl.ds(edge, EDGE), :], hx.at[slot], h_send.at[slot], h_recv.at[slot], to_side)

    def out_copy(n):
        return pltpu.make_async_copy(ob.at[n % 2], y.at[n], o_sem.at[n % 2])

    def rest_copy(n, part):
        if part == 0:
            return pltpu.make_async_copy(xc.at[n % SLOT_X, :, pl.ds(2, WIN)], x_rest.at[n - now], rest_sem.at[n - now, 0])
        return pltpu.make_async_copy(hx.at[n % SLOT_H], h_rest.at[n - now], rest_sem.at[n - now, 1])

    def seen(i):
        return i + 2 + jnp.maximum(i - 9, 0) // 4

    def each(i, run):
        lo, hi = seen(i - 1), seen(i)
        run(lo + 1)

        @pl.when(hi > lo + 1)
        def _():
            run(lo + 2)

    def last(i):
        return jnp.minimum(i + EARLY + 1 + jnp.maximum(i, 0) // 4, images - 1)

    def batch(i, run):
        lo, hi = last(i - 1), last(i)

        @pl.when(hi > lo)
        def _():
            run(lo + 1)

        @pl.when(hi > lo + 1)
        def _():
            run(lo + 2)

    def start_a(n):
        @pl.when(n >= SLOT_A)
        def _():
            pl.semaphore_wait(credit_a, 1)
        for win in range(2):
            own_copy(n, win).start()
            mate_copy(n, win).start()

    def start_x(n):
        @pl.when(n >= SLOT_X)
        def _():
            pl.semaphore_wait(credit_x, 1)
        by_size(far, lambda count, first: far_copy(n, far, chip, count, first).start())

    def wait_a(n):
        for win in range(2):
            own_copy(n, win).wait()
            mate_copy(n, win).wait()

    def start_h(n):
        by_size(far, lambda count, first: far_copy(n, far, chip, count, first).wait_send())
        by_size(model, lambda count, first: far_copy(n, model, 1 - chip, count, first).wait_recv())

        @pl.when(n >= SLOT_H)
        def _():
            pl.semaphore_wait(credit_h, 1)
        side_copy(n).start()

    def wait_h(n):
        side_copy(n).wait()

        @pl.when(n >= now)
        def _():
            rest_copy(n, 0).start()
            rest_copy(n, 1).start()

    def part_copy(n):
        return remote(xc.at[n % SLOT_X, chip, pl.ds(2, WIN), pl.ds(edge, EDGE), :], hp.at[n], p_send.at[n], p_recv.at[n], to_side)

    def control(i):
        batch(i, start_a)

        @pl.when(i >= 1)
        def _():
            batch(i - 2, start_x)
        batch(i - 1, wait_a)

        @pl.when(last(i - 1) > last(i - 2) + 1)
        def _():
            do_merge(last(i - 1) - 1, True)
        each(i, start_h)
        each(i - 1, wait_h)

    def free_a(n):
        @pl.when(n < images - SLOT_A)
        def _():
            pl.semaphore_signal(credit_a, inc=1, device_id=to_mate, device_id_type=MESH)

    def free_built(n):
        @pl.when(n < images - SLOT_X)
        def _():
            pl.semaphore_signal(credit_x, inc=1, device_id=to_far, device_id_type=MESH)

        @pl.when(n < images - SLOT_H)
        def _():
            pl.semaphore_signal(credit_h, inc=1, device_id=to_side, device_id_type=MESH)

    def do_merge(n, live):
        merge(n % SLOT_A, chip, place(model), ab, xc.at[jnp.where(live, n % SLOT_X, SLOT_X)], sb.at[jnp.where(live, n % SLOT_S, SLOT_S)])

    def do_build(n):
        build_x3(is_left, xc.at[n % SLOT_X], hx.at[n % SLOT_H], x3, xh)

    w_far.start()
    w_mate.start()
    w_own.start()
    w2_own.start()

    for n in range(3):
        start_a(n)
    w_own.wait()
    w_mate.wait()

    def fill(t, _):
        @pl.when(t < EARLY)
        def _():
            wait_a(t)

        @pl.when(jnp.logical_and(t >= 1, t <= EARLY))
        def _():
            start_x(t - 1)
            part_copy(t - 1).start()

        @pl.when(t + 3 <= EARLY)
        def _():
            start_a(t + 3)

        @pl.when(t == 2)
        def _():
            w_far.wait()
            w_pass.start()

        @pl.when(t == EARLY + 2)
        def _():
            for p in range(3):
                w_side[p].wait()
                w_last[p].start()
        for p in range(3):
            @pl.when(t == 2 + p)
            def _():
                w_side[p].start()

        @pl.when(t == EARLY + 1)
        def _():
            start_h(0)

        @pl.when(t == EARLY + 2)
        def _():
            start_h(1)

        @pl.when(jnp.logical_and(t >= 2, t < EARLY + 2))
        def _():
            part_copy(t - 2).wait()

        def build_part(n):
            build_half(is_left, xc.at[n % SLOT_X, chip], hp.at[n], x3.at[chip], xh.at[chip])

        @pl.when(t < 3)
        def _():
            do_merge(t, True)

        @pl.when(t == 2)
        def _():
            build_part(0)

        @pl.when(t >= 3)
        def _():
            conv1_part(x3.at[chip], xh.at[chip], w1v.at[chip], zp.at[t - 3])
            build_part(jnp.minimum(t - 2, EARLY - 1))
            do_merge(jnp.minimum(t, EARLY - 1), t < EARLY)

        @pl.when(t < EARLY)
        def _():
            free_a(t)
        return 0

    lax.fori_loop(0, EARLY + 3, fill, 0)
    w2_own.wait()
    for copy in [w_pass] + w_last:
        copy.wait()
    wait_h(0)
    do_build(0)
    free_built(0)
    w_out = pltpu.make_async_copy(w1v, w1_all, w_loc.at[2])
    w_out.start()

    def step(early, i, _):
        control(i)

        @pl.when(i >= 2)
        def _():
            out_copy(i - 2).wait()
        if early:
            conv1(is_left, model == 0, model == 3, [x3.at[1 - chip]], [xh.at[1 - chip]], w1v.at[1 - chip], 1152, b1, y3, zp.at[i])
        else:
            conv1(is_left, model == 0, model == 3, [x3.at[0], x3.at[1]], [xh.at[0], xh.at[1]], w1v, 2304, b1, y3)
        do_build(i + 1)
        do_merge(last(i - 1), last(i - 1) > last(i - 2))
        conv2(y3, w2v, b2, ob.at[i % 2])
        out_copy(i).start()

        batch(i - 1, free_a)
        free_built(i + 1)
        return 0

    lax.fori_loop(0, EARLY, functools.partial(step, True), 0)
    lax.fori_loop(EARLY, now, functools.partial(step, False), 0)
    each(now - 1, wait_h)
    out_copy(now - 2).wait()
    out_copy(now - 1).wait()
    w_out.wait()
    for n in range(now, images):
        rest_copy(n, 0).wait()
        rest_copy(n, 1).wait()


def rest_kernel(images, y_done, x_rest, h_rest, w1, b1, w2, b2, y, xc, hx, x3, xh, y3, ob, w1v, w2v, cb,
                l_sem, w_sem, o_sem, in_sem, out_sem):
    done = images - LATER
    sets = LATER - 1
    size = -(-done // sets)
    model = lax.axis_index('model')
    is_left = lax.axis_index('cols') == 0
    weights = [pltpu.make_async_copy(w1, w1v, w_sem.at[0]), pltpu.make_async_copy(w2, w2v, w_sem.at[1])]
    xh[...] = jnp.zeros_like(xh)

    def load(n):
        return [pltpu.make_async_copy(x_rest.at[n], xc.at[n, :, pl.ds(2, WIN)], l_sem.at[n, 0]),
                pltpu.make_async_copy(h_rest.at[n], hx.at[n], l_sem.at[n, 1])]

    def bring(s, q):
        return pltpu.make_async_copy(y_done.at[s + sets * q], cb.at[s % 2, q], in_sem.at[s % 2, q])

    def put(s, q):
        return pltpu.make_async_copy(cb.at[s % 2, q], y.at[s + sets * q], out_sem.at[s % 2, q])

    def each(s, run):
        for q in range(size):
            @pl.when(jnp.logical_and(jnp.logical_and(s >= 0, s < sets), s + sets * q < done))
            def _():
                run(s, q)

    def out_copy(n):
        return pltpu.make_async_copy(ob.at[n % 2], y.at[done + n], o_sem.at[n % 2])

    for copy in load(0) + weights[:1] + load(1) + weights[1:] + [c for n in range(2, LATER) for c in load(n)]:
        copy.start()
    for copy in load(0):
        copy.wait()
    build_x3(is_left, xc.at[0], hx.at[0], x3, xh)
    for copy in weights:
        copy.wait()

    def step(i, _):
        for n in range(1, LATER):
            @pl.when(i == n - 1)
            def _():
                for copy in load(n):
                    copy.wait()
        each(i - 1, lambda s, q: bring(s, q).wait())
        each(i - 1, lambda s, q: put(s, q).start())
        each(i - 2, lambda s, q: put(s, q).wait())
        each(i, lambda s, q: bring(s, q).start())

        @pl.when(i >= 2)
        def _():
            out_copy(i - 2).wait()
        conv1(is_left, model == 0, model == 3, [x3.at[0], x3.at[1]], [xh.at[0], xh.at[1]], w1v, 2304, b1, y3)
        n = jnp.minimum(i + 1, LATER - 1)
        build_x3(is_left, xc.at[n], hx.at[n], x3, xh)
        conv2(y3, w2v, b2, ob.at[i % 2])
        out_copy(i).start()
        return 0

    lax.fori_loop(0, LATER, step, 0)
    each(jnp.int32(sets - 1), lambda s, q: put(s, q).wait())
    out_copy(LATER - 2).wait()
    out_copy(LATER - 1).wait()


def rest(images, y_done, x_rest, h_rest, w1, b1, w2, b2):
    hbm = pl.BlockSpec(memory_space=pl.ANY)
    vmem = pl.BlockSpec(memory_space=pltpu.VMEM)
    dma = pltpu.SemaphoreType.DMA
    bf16 = jnp.bfloat16
    size = -(-(images - LATER) // (LATER - 1))
    return pl.pallas_call(
        functools.partial(rest_kernel, images),
        out_shape=jax.ShapeDtypeStruct((images, ROWS * COLS, 512), jnp.float32),
        in_specs=[hbm, hbm, hbm, hbm, vmem, hbm, vmem],
        out_specs=hbm,
        scratch_shapes=[
            pltpu.VMEM((LATER, 2, WIN + 4, COLS, 128), bf16),
            pltpu.VMEM((LATER, 2, WIN, EDGE, 128), bf16),
            pltpu.VMEM((2, WIN * COLS, 384), bf16),
            pltpu.VMEM((2, 40, 384), jnp.float32),
            pltpu.VMEM(((ROWS + 2) * COLS, 1536), bf16),
            pltpu.VMEM((2, ROWS * COLS, 512), jnp.float32),
            pltpu.VMEM((2, 9, 128, 512), bf16),
            pltpu.VMEM((4608, 512), bf16),
            pltpu.VMEM((2, size, ROWS * COLS, 512), jnp.float32),
            dma((LATER, 2)), dma((2,)), dma((2,)), dma((2, size)), dma((2, size)),
        ],
        compiler_params=pltpu.CompilerParams(vmem_limit_bytes=62 * 1024 * 1024),
    )(y_done, x_rest, h_rest, w1, b1, w2, b2)


def fused(x, w1, b1, w2, b2):
    images = x.shape[0]
    hbm = pl.BlockSpec(memory_space=pl.ANY)
    vmem = pl.BlockSpec(memory_space=pltpu.VMEM)
    dma = pltpu.SemaphoreType.DMA
    bf16 = jnp.bfloat16
    return pl.pallas_call(
        functools.partial(fused_kernel, images),
        out_shape=[
            jax.ShapeDtypeStruct((images - LATER, ROWS * COLS, 512), jnp.float32),
            jax.ShapeDtypeStruct((LATER, 2, WIN, COLS, 128), bf16),
            jax.ShapeDtypeStruct((LATER, 2, WIN, EDGE, 128), bf16),
            jax.ShapeDtypeStruct((2, 9, 128, 512), bf16),
        ],
        in_specs=[hbm, hbm, vmem, hbm, vmem],
        out_specs=[hbm] * 4,
        scratch_shapes=[
            pltpu.VMEM((SLOT_A, 2, 2, WIN, COLS, 64), bf16),
            pltpu.VMEM((SLOT_S + 1, WIN, COLS, 128), bf16),
            pltpu.VMEM((SLOT_X + 1, 2, WIN + 4, COLS, 128), bf16),
            pltpu.VMEM((SLOT_H, 2, WIN, EDGE, 128), bf16),
            pltpu.VMEM((2, WIN * COLS, 384), bf16),
            pltpu.VMEM((2, 40, 384), jnp.float32),
            pltpu.VMEM(((ROWS + 2) * COLS, 1536), bf16),
            pltpu.VMEM((2, ROWS * COLS, 512), jnp.float32),
            pltpu.VMEM((2, 9, 128, 512), bf16),
            pltpu.VMEM((4608, 512), bf16),
            pltpu.VMEM((EARLY, WIN, EDGE, 128), bf16),
            pltpu.VMEM((EARLY, HALO + (ROWS + 2) * COLS, 512), bf16),
            dma((SLOT_A, 2)), dma((SLOT_A, 2)), dma((SLOT_A, 2)),
            dma((SLOT_X,)), dma((SLOT_X,)), dma((SLOT_H,)), dma((SLOT_H,)), dma((2,)),
            dma((3,)), dma((9,)), dma((9,)), dma((LATER, 2)), dma((EARLY,)), dma((EARLY,)),
            pltpu.SemaphoreType.REGULAR, pltpu.SemaphoreType.REGULAR, pltpu.SemaphoreType.REGULAR,
        ],
        compiler_params=pltpu.CompilerParams(vmem_limit_bytes=60 * 1024 * 1024, collective_id=0, has_side_effects=True),
    )(x, w1, b1, w2, b2)


def solution(mesh):
    def local_step(x, w1, b1, w2, b2):
        images = x.shape[0]
        b1, w2, b2 = b1.reshape(1, 512), w2.reshape(4608, 512), b2.reshape(1, 512)
        done, x_rest, h_rest, w1_all = fused(x, w1.reshape(9, 64, 512), b1, w2, b2)
        y = rest(images, done, x_rest, h_rest, w1_all, b1, w2, b2)
        return y.reshape(images, ROWS, COLS, 512)

    return jax.shard_map(local_step, mesh=mesh, in_specs=(P('data', None, 'cols', 'model'), P(None, None, 'model', None), P(), P(), P()), out_specs=P('data', 'model', 'cols', None), check_vma=False)
```
